256 devices in a mesh: groups: 2 (over z), seq: 128 (over y, x, core).
Axes of the slice: x: 8, y: 8, z: 2, core: 2. Of those that a mesh axis runs over, the one named last changes fastest.
The devices are a block of a 8x8x16 slice.
Arguments:
- queries: bfloat16 [8192, 2048], P(('groups', 'seq')), parts along dimension 0, may hold values from -132 to 132
- fresh_keys: bfloat16 [8192, 2048], P(('groups', 'seq')), parts along dimension 0, may hold values from -6 to 6
- fresh_values: bfloat16 [8192, 2048], P(('groups', 'seq')), parts along dimension 0, may hold values from -48 to 48
- stale_keys: bfloat16 [8192, 2048], P(('groups', 'seq')), parts along dimension 0, may hold values from -6 to 6
- stale_values: bfloat16 [8192, 2048], P(('groups', 'seq')), parts along dimension 0, may hold values from -48 to 48
- patch_sizes: int32 [8], P('groups'), parts along dimension 0, may hold values from 1 to 2048, 4096 in all
Outputs:
- attended: bfloat16 [8192, 2048], P(('groups', 'seq')), parts along dimension 0
The draws below stay inside these ranges and needn't reach their ends.
There are 2 independent parts, one for each index of `groups`. The reference program is written for one: setup_inputs(seed, part) draws one part's arguments, and reference() takes and returns one part's arrays. A program takes and returns all parts, laid end to end along the dimension named above; each array names one. Nothing has to cross between parts.
Inputs may be any that keep to these rules, and one draw needn't show every extreme that they name: `patch_sizes`: the patch lengths sum to 4096.
All inputs are finite; a program needn't handle non-finite values.
Results may differ from the reference program's by a relative error of at most 0.006.
Values may be sent and summed in bfloat16 or wider, within the bound.
A program may use at most 64 MiB of HBM per device.

```python
import math
import jax
import jax.numpy as jnp
import numpy as np
from jax import lax

H = 16
HD = 128
PATCHES = 4
TOKENS = 4096


def base_keys(key):
    return jnp.clip(jax.random.normal(jax.random.fold_in(key, 5), (TOKENS, H * HD), jnp.float32), -6.0, 6.0)


def draw_fresh_keys(key, part):
    return base_keys(key).astype(jnp.bfloat16)


def draw_queries(key, part):
    drawn = jnp.clip(2.0 * jax.random.normal(jax.random.fold_in(key, 6), (TOKENS, H * HD), jnp.float32), -12.0, 12.0)
    return drawn.astype(jnp.bfloat16)


def block_levels(stream_key, shape, cuts, least, high):
    level = 1.0
    for axis_at, shards_of in cuts:
        steps = jax.random.uniform(jax.random.fold_in(jax.random.fold_in(stream_key, 6), axis_at), (shards_of,), jnp.float32, least / len(cuts), high / len(cuts))
        level = level * jnp.repeat(jnp.exp(steps), shape[axis_at] // shards_of).reshape((-1,) + (1,) * (len(shape) - 1 - axis_at))
    return level


def profile(number_of, total, limit, lean):
    loads = [(1 << 20) // math.isqrt(rank ** lean) + 1 for rank in range(2, number_of + 1)]
    spare, holding = total - limit - (number_of - 1), [1] * (number_of - 1)
    while spare > 0:
        free = [i for i in range(number_of - 1) if holding[i] < limit]
        mass, remaining = sum([loads[i] for i in free]), spare
        for i in free:
            more = min(limit - holding[i], max(1, remaining * loads[i] // mass), spare)
            holding[i] = holding[i] + more
            spare = spare - more
    return np.array([limit] + holding)


def ragged_sizes(rng, number_of, total, most, slope):
    if number_of == 2:
        one = jax.random.randint(rng, (), max(1, total - most), min(most, total - 1) + 1)
        return jnp.stack([one, total - one])
    sizes = jnp.asarray(profile(number_of, total, most, slope), jnp.int32)
    couples = (number_of - 1) // 2
    source_of, receiver = sizes[1:1 + 2 * couples:2], sizes[2:2 + 2 * couples:2]
    room = jnp.minimum(source_of - 1, most - receiver)
    moved = jax.random.randint(jax.random.fold_in(rng, 1), (couples,), 0, 1 << 20) % (room + 1)
    sizes = sizes.at[1:1 + 2 * couples:2].set(source_of - moved).at[2:2 + 2 * couples:2].set(receiver + moved)
    return sizes[jax.random.permutation(jax.random.fold_in(rng, 2), number_of)]


def scatter_about(own_key, extent, spread, bound, split=(), held_as=jnp.bfloat16):
    entries = jax.random.normal(own_key, extent, jnp.float32) * spread
    if len(split) > 0:
        entries = block_levels(own_key, extent, split, -0.22, 0.18) * entries
    return jnp.clip(entries, min=-bound, max=bound).astype(held_as)


def setup_inputs(seed: int = 0, part: int = 0) -> dict:
    arg_keys = jax.random.split(jax.random.key(seed), 7)
    part_keys = jax.random.split(jax.random.fold_in(arg_keys[6], part), 7)
    queries = draw_queries(jax.random.fold_in(jax.random.fold_in(arg_keys[6], part), 71), part)
    fresh_keys = draw_fresh_keys(jax.random.fold_in(jax.random.fold_in(arg_keys[6], part), 71), part)
    fresh_values = scatter_about(part_keys[2], (TOKENS, H * HD), 8.0, 48.0, ((0, 128),))
    stale_keys = scatter_about(part_keys[3], (TOKENS, H * HD), 1.0, 6.0, ((0, 128),))
    stale_values = scatter_about(part_keys[4], (TOKENS, H * HD), 8.0, 48.0, ((0, 128),))
    patch_sizes = ragged_sizes(part_keys[5], PATCHES, TOKENS, TOKENS // 2, 1).astype(jnp.int32)
    return dict(queries=queries, fresh_keys=fresh_keys, fresh_values=fresh_values, stale_keys=stale_keys, stale_values=stale_values, patch_sizes=patch_sizes)


def reference(queries, fresh_keys, fresh_values, stale_keys, stale_values, patch_sizes):
    total_rows, columns = queries.shape
    head_size = columns // H
    block_rows = math.gcd(total_rows, 512)
    patch_ends = jnp.cumsum(patch_sizes)[:-1]
    positions = jnp.arange(total_rows, dtype=jnp.int32)
    token_patch = jnp.sum((positions[:, None] >= patch_ends[None, :]).astype(jnp.int32), axis=1)
    score_scale = head_size ** -0.5

    def one_head(head):
        start = (head * head_size).astype(jnp.int32)

        def take(array):
            return lax.dynamic_slice_in_dim(array, start, head_size, 1)

        query_head = take(queries).reshape(-1, block_rows, head_size)
        key_fresh = take(fresh_keys)
        value_fresh = take(fresh_values)
        key_stale = take(stale_keys)
        value_stale = take(stale_values)
        patch_blocks = token_patch.reshape(-1, block_rows)

        def one_block(pair):
            query_block, query_patch = pair
            is_fresh = token_patch[None, :] <= query_patch[:, None]
            fresh_scores = jnp.dot(query_block, key_fresh.T, preferred_element_type=jnp.float32)
            stale_scores = jnp.dot(query_block, key_stale.T, preferred_element_type=jnp.float32)
            scores = jnp.where(is_fresh, fresh_scores, stale_scores) * score_scale
            weights = jnp.exp(scores - jnp.max(scores, axis=1, keepdims=True))
            denominator = jnp.sum(weights, axis=1, keepdims=True)
            rounded = weights.astype(jnp.bfloat16)
            zeroes = jnp.zeros_like(rounded)
            numerator = jnp.dot(jnp.where(is_fresh, rounded, zeroes), value_fresh, preferred_element_type=jnp.float32)
            numerator = numerator + jnp.dot(jnp.where(is_fresh, zeroes, rounded), value_stale, preferred_element_type=jnp.float32)
            return (numerator / denominator).astype(jnp.bfloat16)

        return lax.map(one_block, (query_head, patch_blocks)).reshape(total_rows, head_size)

    heads_out = lax.map(one_head, jnp.arange(H, dtype=jnp.int32))
    return jnp.transpose(heads_out, (1, 0, 2)).reshape(total_rows, columns)
```

```python
import functools
import math

import jax
import jax.numpy as jnp
from jax import lax
from jax.experimental import pallas as pl
from jax.experimental.pallas import tpu as pltpu
from jax.sharding import PartitionSpec as P

HEAD = 128
SUBS = 4
MESH = pl.DeviceIdType.MESH


def kernel(
    side,
    local,
    sizes,
    q_in,
    fk_in,
    fv_in,
    sk_in,
    sv_in,
    out,
    stage,
    qall,
    kv,
    vaug,
    opart,
    lpart,
    orecv,
    lrecv,
    outst,
    load_sem,
    self_sem,
    p1_send,
    p1_recv,
    ring_send,
    ring_recv,
    part_send,
    part_recv,
    p4_send,
    p4_recv,
):
    group = lax.axis_index("groups")
    me = lax.axis_index("seq")
    c = me % 2
    x = (me // 2) % side
    y = me // 2 // side
    a = x * (1 - c) + y * c
    g = y * (1 - c) + x * c
    rows = 2 * side * local
    half = side // 2
    pair = 2 * local
    scale2 = (HEAD**-0.5) * math.log2(math.e)

    def at(cx, cy, core):
        return (group, (cy * side + cx) * 2 + core)

    def line(a_to, g_to, core):
        return at(a_to * (1 - c) + g_to * c, g_to * (1 - c) + a_to * c, core)

    def head_cols(head):
        return pl.ds(pl.multiple_of(head * HEAD, HEAD), HEAD)

    loads = []
    for i, ref in enumerate((q_in, fk_in, fv_in, sk_in, sv_in)):
        loads.append(pltpu.make_async_copy(ref, stage.at[i], load_sem.at[i]))
        loads[-1].start()

    barrier = pltpu.get_barrier_semaphore()
    for j in range(1, side):
        for core in range(2):
            pl.semaphore_signal(barrier, inc=1, device_id=at((x + j) % side, y, core), device_id_type=MESH)
            pl.semaphore_signal(barrier, inc=1, device_id=at(x, (y + j) % side, core), device_id_type=MESH)
    pl.semaphore_signal(barrier, inc=1, device_id=at(x, y, 1 - c), device_id_type=MESH)

    own_row = pl.ds(pl.multiple_of((a * 2 + c) * local, local), local)
    own_head = c * side + a
    own = []
    for i, ref in enumerate((q_in, fk_in, fv_in, sk_in, sv_in)):
        dst = qall.at[g, own_row, :] if i == 0 else kv.at[i - 1, own_row, :]
        own.append(pltpu.make_async_copy(ref.at[:, head_cols(own_head)], dst, self_sem.at[i]))
        own[-1].start()
    vaug[:, HEAD:] = jnp.ones((2 * rows, HEAD), jnp.bfloat16)

    for copy in loads:
        copy.wait()
    pl.semaphore_wait(barrier, 4 * (side - 1) + 1)

    row_x = pl.ds(pl.multiple_of((x * 2 + c) * local, local), local)
    row_y = pl.ds(pl.multiple_of((y * 2 + c) * local, local), local)

    order = []
    for j in range(1, half + 1):
        order.append(j)
        if j != side - j:
            order.append(side - j)

    def send_slices(which):
        def go(device, head, slot, row):
            if which == 0:
                src, dst = stage.at[0, :, head_cols(head)], qall.at[slot, row, :]
            else:
                src, dst = stage.at[pl.ds(1, 4), :, head_cols(head)], kv.at[:, row, :]
            pltpu.make_async_remote_copy(
                src_ref=src,
                dst_ref=dst,
                send_sem=p1_send.at[which],
                recv_sem=p1_recv.at[which],
                device_id=device,
                device_id_type=MESH,
            ).start()

        for j in order:
            to_x, to_y = (x + j) % side, (y + j) % side
            go(at(to_x, y, 0), to_x, y, row_x)
            go(at(x, to_y, 1), side + to_y, x, row_y)
        d = 1 - c
        go(
            at(x, y, d),
            d * side + x * (1 - d) + y * d,
            y * (1 - d) + x * d,
            pl.ds(pl.multiple_of(((x * (1 - d) + y * d) * 2 + c) * local, local), local),
        )

    send_slices(0)
    send_slices(1)

    sub_rows = rows // SUBS

    def subs_of(direction, step):
        if step < half:
            return list(range(SUBS))
        return list(range(SUBS // 2)) if direction == 0 else list(range(SUBS // 2, SUBS))

    def sub_ref(chunk, sub):
        return qall.at[chunk, pl.ds(sub * sub_rows, sub_rows), :]

    def ring(direction, step, sub):
        if direction == 0:
            chunk, to = (g + side - (step - 1)) % side, (g + 1) % side
        else:
            chunk, to = (g + step - 1) % side, (g + side - 1) % side
        return pltpu.make_async_remote_copy(
            src_ref=sub_ref(chunk, sub),
            dst_ref=sub_ref(chunk, sub),
            send_sem=ring_send.at[direction, step - 1, sub],
            recv_sem=ring_recv.at[direction, step - 1, sub],
            device_id=line(a, to, c),
            device_id_type=MESH,
        )

    def ring_wait(direction, step, sub):
        chunk = (g + side - step) % side if direction == 0 else (g + step) % side
        ref = sub_ref(chunk, sub)
        pltpu.make_async_copy(ref, ref, ring_recv.at[direction, step - 1, sub]).wait()

    sent = []

    def ring_start(step):
        for sub in range(SUBS):
            for direction in range(2):
                if step > 1 and step - 1 < half:
                    ring_wait(direction, step - 1, sub)
                if step <= half and sub in subs_of(direction, step):
                    copy = ring(direction, step, sub)
                    copy.start()
                    sent.append(copy)

    own[0].wait()
    others = rows - local
    ref = qall.at[0, pl.ds(0, others), :]
    pltpu.make_async_copy(ref, ref, p1_recv.at[0]).wait()
    ring_start(1)
    ring_start(2)

    for copy in own[1:]:
        copy.wait()
    ref = kv.at[:, pl.ds(0, others), :]
    pltpu.make_async_copy(ref, ref, p1_recv.at[1]).wait()
    vaug[pl.ds(0, rows), pl.ds(0, HEAD)] = kv[1]
    vaug[pl.ds(rows, rows), pl.ds(0, HEAD)] = kv[3]

    step_a = pair * (1 + c * (side - 1))
    step_g = pair * (side - c * (side - 1))
    end0 = sizes[0]
    end1 = end0 + sizes[1]
    end2 = end1 + sizes[2]
    big = jnp.int32(2**30)

    def position(l, chunk):
        return (l // pair) * step_a + chunk * step_g + l % pair

    key_pos = position(lax.broadcasted_iota(jnp.int32, (8, rows), 1), g)[0:1, :]
    eye = lax.broadcasted_iota(jnp.int32, (HEAD, HEAD), 0) == lax.broadcasted_iota(jnp.int32, (HEAD, HEAD), 1)
    contract = (((1,), (1,)), ((), ()))
    qt = min(256, rows)

    def compute(chunk, o_ref, l_ref):
        def tile(t, _):
            start = pl.multiple_of(t * qt, qt)
            q = qall[chunk, pl.ds(start, qt), :]
            pos = position(lax.broadcasted_iota(jnp.int32, (qt, HEAD), 0) + start, chunk)
            thr = jnp.where(pos < end0, end0, jnp.where(pos < end1, end1, jnp.where(pos < end2, end2, big)))
            thr = jnp.concatenate([thr] * (rows // HEAD), axis=1)
            fresh = key_pos < thr
            sf = lax.dot_general(q, kv[0], contract, preferred_element_type=jnp.float32)
            ss = lax.dot_general(q, kv[2], contract, preferred_element_type=jnp.float32)
            s = jnp.where(fresh, sf, ss)
            m = jnp.max(s, axis=1, keepdims=True)
            p = jnp.exp2((s - m) * scale2)
            pf = jnp.where(fresh, p, 0.0)
            both = jnp.concatenate([pf.astype(jnp.bfloat16), (p - pf).astype(jnp.bfloat16)], axis=1)
            o = jnp.dot(both, vaug[...], preferred_element_type=jnp.float32)
            total = o[:, HEAD:]
            o_ref[pl.ds(start, qt), :] = (o[:, :HEAD] / total).astype(jnp.bfloat16)
            lse = m * scale2 + jnp.log2(total)
            for k in range(qt // HEAD):
                block = lse[k * HEAD : (k + 1) * HEAD, :]
                l_ref[pl.ds(t * (qt // HEAD) + k, 1), :] = jnp.sum(jnp.where(eye, block, 0.0), axis=0, keepdims=True)
            return 0

        lax.fori_loop(0, rows // qt, tile, 0)

    def part_copies(delta):
        to = line(a, (g + side - delta) % side, c)
        kinds = ((opart, orecv), (lpart, lrecv))
        return [
            pltpu.make_async_remote_copy(
                src_ref=src.at[delta],
                dst_ref=dst.at[delta],
                send_sem=part_send.at[kind, delta],
                recv_sem=part_recv.at[kind, delta],
                device_id=to,
                device_id_type=MESH,
            )
            for kind, (src, dst) in enumerate(kinds)
        ]

    def do_part(delta):
        compute((g + side - delta) % side, opart.at[delta], lpart.at[delta])
        for copy in part_copies(delta):
            copy.start()
            sent.append(copy)

    compute(g, orecv.at[0], lrecv.at[0])
    for step in range(1, half):
        ring_start(step + 2)
        do_part(step)
        do_part(side - step)
    for direction in range(2):
        for sub in subs_of(direction, half):
            ring_wait(direction, half, sub)
    do_part(half)

    for delta in range(1, side):
        for kind, ref in enumerate((orecv, lrecv)):
            pltpu.make_async_copy(ref.at[delta], ref.at[delta], part_recv.at[kind, delta]).wait()
    lse = [lrecv[delta] for delta in range(side)]
    top = functools.reduce(jnp.maximum, lse)
    weights = [jnp.exp2(l - top) for l in lse]
    total = functools.reduce(jnp.add, weights)
    weights = [w / total for w in weights]
    for t in range(rows // HEAD):
        acc = jnp.zeros((HEAD, HEAD), jnp.float32)
        for delta in range(side):
            w = jnp.sum(jnp.where(eye, weights[delta][t : t + 1, :], 0.0), axis=1, keepdims=True)
            acc = acc + w * orecv[delta, pl.ds(t * HEAD, HEAD), :].astype(jnp.float32)
        outst[pl.ds(t * HEAD, HEAD), :] = acc.astype(jnp.bfloat16)

    def home(a_to, core):
        row = pl.ds(pl.multiple_of((a_to * 2 + core) * local, local), local)
        pltpu.make_async_remote_copy(
            src_ref=outst.at[row, :],
            dst_ref=out.at[:, head_cols(own_head)],
            send_sem=p4_send,
            recv_sem=p4_recv,
            device_id=line(a_to, g, core),
            device_id_type=MESH,
        ).start()

    for j in order:
        for core in range(2):
            home((a + j) % side, core)
    home(a, 1 - c)
    out[:, head_cols(own_head)] = outst[own_row, :]

    ref = qall.at[0, pl.ds(0, others), :]
    pltpu.make_async_copy(ref, ref, p1_send.at[0]).wait()
    ref = kv.at[:, pl.ds(0, others), :]
    pltpu.make_async_copy(ref, ref, p1_send.at[1]).wait()
    for copy in sent:
        copy.wait_send()
    ref = outst.at[pl.ds(0, others), :]
    pltpu.make_async_copy(ref, ref, p4_recv).wait()
    pltpu.make_async_copy(ref, ref, p4_send).wait()


def shards(queries, fresh_keys, fresh_values, stale_keys, stale_values, patch_sizes):
    local, columns = queries.shape
    chips = lax.axis_size("seq") // 2
    side = math.isqrt(chips)
    assert side * side == chips and columns == 2 * side * HEAD
    rows = 2 * side * local
    half = side // 2
    bf16, f32 = jnp.bfloat16, jnp.float32
    dma = pltpu.SemaphoreType.DMA
    return pl.pallas_call(
        functools.partial(kernel, side, local),
        out_shape=jax.ShapeDtypeStruct((local, columns), bf16),
        in_specs=[pl.BlockSpec(memory_space=pltpu.SMEM)] + [pl.BlockSpec(memory_space=pl.ANY)] * 5,
        out_specs=pl.BlockSpec(memory_space=pltpu.VMEM),
        scratch_shapes=[
            pltpu.VMEM((5, local, columns), bf16),
            pltpu.VMEM((side, rows, HEAD), bf16),
            pltpu.VMEM((4, rows, HEAD), bf16),
            pltpu.VMEM((2 * rows, 2 * HEAD), bf16),
            pltpu.VMEM((side, rows, HEAD), bf16),
            pltpu.VMEM((side, rows // HEAD, HEAD), f32),
            pltpu.VMEM((side, rows, HEAD), bf16),
            pltpu.VMEM((side, rows // HEAD, HEAD), f32),
            pltpu.VMEM((rows, HEAD), bf16),
            dma((5,)),
            dma((5,)),
            dma((2,)),
            dma((2,)),
            dma((2, half, SUBS)),
            dma((2, half, SUBS)),
            dma((2, side)),
            dma((2, side)),
            dma,
            dma,
        ],
        compiler_params=pltpu.CompilerParams(collective_id=0, has_side_effects=True),
    )(patch_sizes, queries, fresh_keys, fresh_values, stale_keys, stale_values)


def solution(mesh):
    in_specs = (
        P(("groups", "seq"), None),
        P(("groups", "seq"), None),
        P(("groups", "seq"), None),
        P(("groups", "seq"), None),
        P(("groups", "seq"), None),
        P("groups"),
    )
    out_specs = P(("groups", "seq"), None)
    return jax.shard_map(shards, mesh=mesh, in_specs=in_specs, out_specs=out_specs, check_vma=False)
```

```python
import functools
import math

import jax
import jax.numpy as jnp
from jax import lax
from jax.experimental import pallas as pl
from jax.experimental.pallas import tpu as pltpu
from jax.sharding import PartitionSpec as P

HEAD = 128
SUBS = 4
PATCHES = 4
QT = 512
MESH = pl.DeviceIdType.MESH


def kernel(
    side,
    local,
    sizes,
    q_in,
    fk_in,
    fv_in,
    sk_in,
    sv_in,
    out,
    stage,
    qall,
    kv,
    kcat,
    vcat,
    opart,
    lpart,
    orecv,
    lrecv,
    outst,
    load_sem,
    self_sem,
    p1_send,
    p1_recv,
    ring_send,
    ring_recv,
    part_send,
    part_recv,
    p4_send,
    p4_recv,
):
    group = lax.axis_index("groups")
    me = lax.axis_index("seq")
    c = me % 2
    x = (me // 2) % side
    y = me // 2 // side
    a = x * (1 - c) + y * c
    g = y * (1 - c) + x * c
    rows = 2 * side * local
    half = side // 2
    pair = 2 * local
    scale2 = (HEAD**-0.5) * math.log2(math.e)

    def at(cx, cy, core):
        return (group, (cy * side + cx) * 2 + core)

    def line(a_to, g_to, core):
        return at(a_to * (1 - c) + g_to * c, g_to * (1 - c) + a_to * c, core)

    def head_cols(head):
        return pl.ds(pl.multiple_of(head * HEAD, HEAD), HEAD)

    loads = []
    for i, ref in enumerate((q_in, fk_in, fv_in, sk_in, sv_in)):
        loads.append(pltpu.make_async_copy(ref, stage.at[i], load_sem.at[i]))
        loads[-1].start()

    barrier = pltpu.get_barrier_semaphore()
    for j in range(1, side):
        for core in range(2):
            pl.semaphore_signal(barrier, inc=1, device_id=at((x + j) % side, y, core), device_id_type=MESH)
            pl.semaphore_signal(barrier, inc=1, device_id=at(x, (y + j) % side, core), device_id_type=MESH)
    pl.semaphore_signal(barrier, inc=1, device_id=at(x, y, 1 - c), device_id_type=MESH)

    own_row = pl.ds(pl.multiple_of((a * 2 + c) * local, local), local)
    own_head = c * side + a
    own = []
    for i, ref in enumerate((q_in, fk_in, fv_in, sk_in, sv_in)):
        dst = qall.at[g, own_row, :] if i == 0 else kv.at[i - 1, own_row, :]
        own.append(pltpu.make_async_copy(ref.at[:, head_cols(own_head)], dst, self_sem.at[i]))
        own[-1].start()

    for copy in loads:
        copy.wait()
    pl.semaphore_wait(barrier, 4 * (side - 1) + 1)

    row_x = pl.ds(pl.multiple_of((x * 2 + c) * local, local), local)
    row_y = pl.ds(pl.multiple_of((y * 2 + c) * local, local), local)

    order = []
    for j in range(1, half + 1):
        order.append(j)
        if j != side - j:
            order.append(side - j)

    def send_slices(which):
        def go(device, head, slot, row):
            if which == 0:
                src, dst = stage.at[0, :, head_cols(head)], qall.at[slot, row, :]
            else:
                src, dst = stage.at[pl.ds(1, 4), :, head_cols(head)], kv.at[:, row, :]
            pltpu.make_async_remote_copy(
                src_ref=src,
                dst_ref=dst,
                send_sem=p1_send.at[which],
                recv_sem=p1_recv.at[which],
                device_id=device,
                device_id_type=MESH,
            ).start()

        for j in order:
            to_x, to_y = (x + j) % side, (y + j) % side
            go(at(to_x, y, 0), to_x, y, row_x)
            go(at(x, to_y, 1), side + to_y, x, row_y)
        d = 1 - c
        go(
            at(x, y, d),
            d * side + x * (1 - d) + y * d,
            y * (1 - d) + x * d,
            pl.ds(pl.multiple_of(((x * (1 - d) + y * d) * 2 + c) * local, local), local),
        )

    send_slices(0)
    send_slices(1)

    sub_rows = rows // SUBS

    def subs_of(direction, step):
        if step < half:
            return list(range(SUBS))
        return list(range(SUBS // 2)) if direction == 0 else list(range(SUBS // 2, SUBS))

    def sub_ref(chunk, sub):
        return qall.at[chunk, pl.ds(sub * sub_rows, sub_rows), :]

    def ring(direction, step, sub):
        if direction == 0:
            chunk, to = (g + side - (step - 1)) % side, (g + 1) % side
        else:
            chunk, to = (g + step - 1) % side, (g + side - 1) % side
        return pltpu.make_async_remote_copy(
            src_ref=sub_ref(chunk, sub),
            dst_ref=sub_ref(chunk, sub),
            send_sem=ring_send.at[direction, step - 1, sub],
            recv_sem=ring_recv.at[direction, step - 1, sub],
            device_id=line(a, to, c),
            device_id_type=MESH,
        )

    def ring_wait(direction, step, sub):
        chunk = (g + side - step) % side if direction == 0 else (g + step) % side
        ref = sub_ref(chunk, sub)
        pltpu.make_async_copy(ref, ref, ring_recv.at[direction, step - 1, sub]).wait()

    sent = []

    def ring_start(step):
        for sub in range(SUBS):
            for direction in range(2):
                if step > 1 and step - 1 < half:
                    ring_wait(direction, step - 1, sub)
                if step <= half and sub in subs_of(direction, step):
                    copy = ring(direction, step, sub)
                    copy.start()
                    sent.append(copy)

    own[0].wait()
    others = rows - local
    ref = qall.at[0, pl.ds(0, others), :]
    pltpu.make_async_copy(ref, ref, p1_recv.at[0]).wait()
    ring_start(1)
    ring_start(2)

    for copy in own[1:]:
        copy.wait()
    ref = kv.at[:, pl.ds(0, others), :]
    pltpu.make_async_copy(ref, ref, p1_recv.at[1]).wait()

    step_a = pair * (1 + c * (side - 1))
    step_g = pair * (side - c * (side - 1))
    end0 = sizes[0]
    end1 = end0 + sizes[1]
    end2 = end1 + sizes[2]

    def patches(count, start, chunk):
        l = lax.broadcasted_iota(jnp.int32, (count, HEAD), 0) + start
        pos = (l // pair) * step_a + chunk * step_g + l % pair
        one, zero = jnp.int32(1), jnp.int32(0)
        return sum(jnp.where(pos >= end, one, zero) for end in (end0, end1, end2))

    def indicator(mask):
        return jnp.where(mask, 1.0, 0.0).astype(jnp.bfloat16)

    key_patch = patches(rows, 0, g)
    for p in range(PATCHES):
        cols = pl.ds(p * HEAD, HEAD)
        fresh, stale = indicator(key_patch <= p), indicator(key_patch > p)
        kcat[:, cols] = kv[0] * fresh + kv[2] * stale
        vcat[:, cols] = kv[1] * fresh + kv[3] * stale

    eye = lax.broadcasted_iota(jnp.int32, (HEAD, HEAD), 0) == lax.broadcasted_iota(jnp.int32, (HEAD, HEAD), 1)
    contract = (((1,), (1,)), ((), ()))
    qt = min(QT, rows)

    def compute(chunk, o_ref, l_ref):
        def tile(t, _):
            start = t * qt if isinstance(t, int) else pl.multiple_of(t * qt, qt)
            q = qall[chunk, pl.ds(start, qt), :]
            patch = patches(qt, start, chunk)
            split = jnp.concatenate([q * indicator(patch == p) for p in range(PATCHES)], axis=1)
            s = lax.dot_general(split, kcat[...], contract, preferred_element_type=jnp.float32)
            m = jnp.max(s, axis=1, keepdims=True)
            w = jnp.exp2((s - m) * scale2)
            total = jnp.sum(w, axis=1, keepdims=True)
            o = jnp.dot(w.astype(jnp.bfloat16), vcat[...], preferred_element_type=jnp.float32)
            picked = o[:, :HEAD]
            for p in range(1, PATCHES):
                picked = jnp.where(patch == p, o[:, p * HEAD : (p + 1) * HEAD], picked)
            o_ref[pl.ds(start, qt), :] = (picked / total).astype(jnp.bfloat16)
            lse = m * scale2 + jnp.log2(total)
            for k in range(qt // HEAD):
                block = lse[k * HEAD : (k + 1) * HEAD, :]
                l_ref[pl.ds(t * (qt // HEAD) + k, 1), :] = jnp.sum(jnp.where(eye, block, 0.0), axis=0, keepdims=True)
            return 0

        if rows == qt:
            tile(0, 0)
        else:
            lax.fori_loop(0, rows // qt, tile, 0)

    def part_copies(delta):
        to = line(a, (g + side - delta) % side, c)
        kinds = ((opart, orecv), (lpart, lrecv))
        return [
            pltpu.make_async_remote_copy(
                src_ref=src.at[delta],
                dst_ref=dst.at[delta],
                send_sem=part_send.at[kind, delta],
                recv_sem=part_recv.at[kind, delta],
                device_id=to,
                device_id_type=MESH,
            )
            for kind, (src, dst) in enumerate(kinds)
        ]

    def do_part(delta):
        compute((g + side - delta) % side, opart.at[delta], lpart.at[delta])
        for copy in part_copies(delta):
            copy.start()
            sent.append(copy)

    compute(g, orecv.at[0], lrecv.at[0])
    for step in range(1, half):
        ring_start(step + 2)
        do_part(step)
        do_part(side - step)
    for direction in range(2):
        for sub in subs_of(direction, half):
            ring_wait(direction, half, sub)
    do_part(half)

    for delta in range(1, side):
        for kind, ref in enumerate((orecv, lrecv)):
            pltpu.make_async_copy(ref.at[delta], ref.at[delta], part_recv.at[kind, delta]).wait()
    lse = [lrecv[delta] for delta in range(side)]
    top = functools.reduce(jnp.maximum, lse)
    weights = [jnp.exp2(l - top) for l in lse]
    total = functools.reduce(jnp.add, weights)
    weights = [w / total for w in weights]
    for t in range(rows // HEAD):
        acc = jnp.zeros((HEAD, HEAD), jnp.float32)
        for delta in range(side):
            w = jnp.sum(jnp.where(eye, weights[delta][t : t + 1, :], 0.0), axis=1, keepdims=True)
            acc = acc + w * orecv[delta, pl.ds(t * HEAD, HEAD), :].astype(jnp.float32)
        outst[pl.ds(t * HEAD, HEAD), :] = acc.astype(jnp.bfloat16)

    def home(a_to, core):
        row = pl.ds(pl.multiple_of((a_to * 2 + core) * local, local), local)
        pltpu.make_async_remote_copy(
            src_ref=outst.at[row, :],
            dst_ref=out.at[:, head_cols(own_head)],
            send_sem=p4_send,
            recv_sem=p4_recv,
            device_id=line(a_to, g, core),
            device_id_type=MESH,
        ).start()

    for j in order:
        for core in range(2):
            home((a + j) % side, core)
    home(a, 1 - c)
    out[:, head_cols(own_head)] = outst[own_row, :]

    ref = qall.at[0, pl.ds(0, others), :]
    pltpu.make_async_copy(ref, ref, p1_send.at[0]).wait()
    ref = kv.at[:, pl.ds(0, others), :]
    pltpu.make_async_copy(ref, ref, p1_send.at[1]).wait()
    for copy in sent:
        copy.wait_send()
    ref = outst.at[pl.ds(0, others), :]
    pltpu.make_async_copy(ref, ref, p4_recv).wait()
    pltpu.make_async_copy(ref, ref, p4_send).wait()


def shards(queries, fresh_keys, fresh_values, stale_keys, stale_values, patch_sizes):
    local, columns = queries.shape
    chips = lax.axis_size("seq") // 2
    side = math.isqrt(chips)
    assert side * side == chips and columns == 2 * side * HEAD
    rows = 2 * side * local
    half = side // 2
    bf16, f32 = jnp.bfloat16, jnp.float32
    dma = pltpu.SemaphoreType.DMA
    return pl.pallas_call(
        functools.partial(kernel, side, local),
        out_shape=jax.ShapeDtypeStruct((local, columns), bf16),
        in_specs=[pl.BlockSpec(memory_space=pltpu.SMEM)] + [pl.BlockSpec(memory_space=pl.ANY)] * 5,
        out_specs=pl.BlockSpec(memory_space=pltpu.VMEM),
        scratch_shapes=[
            pltpu.VMEM((5, local, columns), bf16),
            pltpu.VMEM((side, rows, HEAD), bf16),
            pltpu.VMEM((4, rows, HEAD), bf16),
            pltpu.VMEM((rows, PATCHES * HEAD), bf16),
            pltpu.VMEM((rows, PATCHES * HEAD), bf16),
            pltpu.VMEM((side, rows, HEAD), bf16),
            pltpu.VMEM((side, rows // HEAD, HEAD), f32),
            pltpu.VMEM((side, rows, HEAD), bf16),
            pltpu.VMEM((side, rows // HEAD, HEAD), f32),
            pltpu.VMEM((rows, HEAD), bf16),
            dma((5,)),
            dma((5,)),
            dma((2,)),
            dma((2,)),
            dma((2, half, SUBS)),
            dma((2, half, SUBS)),
            dma((2, side)),
            dma((2, side)),
            dma,
            dma,
        ],
        compiler_params=pltpu.CompilerParams(collective_id=0, has_side_effects=True),
    )(patch_sizes, queries, fresh_keys, fresh_values, stale_keys, stale_values)


def solution(mesh):
    in_specs = (
        P(("groups", "seq"), None),
        P(("groups", "seq"), None),
        P(("groups", "seq"), None),
        P(("groups", "seq"), None),
        P(("groups", "seq"), None),
        P("groups"),
    )
    out_specs = P(("groups", "seq"), None)
    return jax.shard_map(shards, mesh=mesh, in_specs=in_specs, out_specs=out_specs, check_vma=False)
```

```python
import functools
import math

import jax
import jax.numpy as jnp
from jax import lax
from jax.experimental import pallas as pl
from jax.experimental.pallas import tpu as pltpu
from jax.sharding import PartitionSpec as P

HEAD = 128
SUBS = 4
PATCHES = 4
MESH = pl.DeviceIdType.MESH


def kernel(
    side,
    local,
    sizes,
    q_in,
    fk_in,
    fv_in,
    sk_in,
    sv_in,
    out,
    stage,
    qall,
    kv,
    kcat,
    vcat,
    opart,
    lpart,
    orecv,
    lrecv,
    outst,
    load_sem,
    self_sem,
    p1_send,
    p1_recv,
    ready,
    ring_send,
    ring_recv,
    direct_send,
    direct_recv,
    part_send,
    part_recv,
    p4_send,
    p4_recv,
):
    group = lax.axis_index("groups")
    me = lax.axis_index("seq")
    c = me % 2
    x = (me // 2) % side
    y = me // 2 // side
    a = x * (1 - c) + y * c
    g = y * (1 - c) + x * c
    rows = 2 * side * local
    pair = 2 * local
    scale2 = (HEAD**-0.5) * math.log2(math.e)

    def at(cx, cy, core):
        return (group, (cy * side + cx) * 2 + core)

    def line(a_to, g_to, core):
        return at(a_to * (1 - c) + g_to * c, g_to * (1 - c) + a_to * c, core)

    def head_cols(head):
        return pl.ds(pl.multiple_of(head * HEAD, HEAD), HEAD)

    inputs = (q_in, fk_in, fv_in, sk_in, sv_in)
    loads = [pltpu.make_async_copy(ref, stage.at[i], load_sem.at[i]) for i, ref in enumerate(inputs)]
    for copy in loads:
        copy.start()

    def block(index):
        return pl.ds(pl.multiple_of(index * local, local), local)

    def signal(semaphore, device):
        pl.semaphore_signal(semaphore, inc=1, device_id=device, device_id_type=MESH)

    def loop(first, last, body):
        def step(i, carry):
            body(i)
            return carry

        lax.fori_loop(first, last, step, 0)

    barrier = pltpu.get_barrier_semaphore()

    def greet_row(i):
        signal(barrier, at(i, y, 0))
        signal(barrier, at(i, y, 1))

    def greet_column(i):
        signal(barrier, at(x, i, 0))
        signal(barrier, at(x, i, 1))

    loop(0, x, greet_row)
    loop(0, y, greet_column)

    @pl.when(c == 1)
    def _():
        signal(barrier, at(x, y, 0))

    own_row = block(a * 2 + c)
    own_head = c * side + a
    own = []
    for i, ref in enumerate(inputs):
        dst = qall.at[g, own_row, :] if i == 0 else kv.at[i - 1, own_row, :]
        own.append(pltpu.make_async_copy(ref.at[:, head_cols(own_head)], dst, self_sem.at[i]))
        own[-1].start()

    higher = 2 * (side - 1 - x) + 2 * (side - 1 - y) + (1 - c)

    @pl.when(higher > 0)
    def _():
        pl.semaphore_wait(barrier, higher)

    def ready_row(i):
        signal(ready.at[x * 2 + c], at(i, y, 0))
        signal(ready.at[x * 2 + c], at(i, y, 1))

    def ready_column(i):
        signal(ready.at[2 * side + y * 2 + c], at(x, i, 0))
        signal(ready.at[2 * side + y * 2 + c], at(x, i, 1))

    loop(x + 1, side, ready_row)
    loop(y + 1, side, ready_column)

    @pl.when(c == 0)
    def _():
        signal(ready.at[x * 2], at(x, y, 1))

    row_x, row_y = block(x * 2 + c), block(y * 2 + c)

    def push(which, device, head, slot, row):
        if which == 0:
            src, dst = stage.at[0, :, head_cols(head)], qall.at[slot, row, :]
        else:
            src, dst = stage.at[pl.ds(1, 4), :, head_cols(head)], kv.at[:, row, :]
        pltpu.make_async_remote_copy(
            src_ref=src,
            dst_ref=dst,
            send_sem=p1_send.at[which],
            recv_sem=p1_recv.at[which],
            device_id=device,
            device_id_type=MESH,
        ).start()

    def push_row(which, i):
        push(which, at(i, y, 0), i, y, row_x)

    def push_column(which, i):
        push(which, at(x, i, 1), side + i, x, row_y)

    for which in range(2):
        for copy in loads[:1] if which == 0 else loads[1:]:
            copy.wait()
        loop(x + 1, side, functools.partial(push_row, which))
        loop(y + 1, side, functools.partial(push_column, which))

        @pl.when(c == 0)
        def _():
            push_column(which, y)

    def hear(index):
        pl.semaphore_wait(ready.at[index], 1)

    def lower_row(k):
        i = x - 1 - k

        @pl.when(i + y > 0)
        def _():
            hear(i * 2)
            hear(i * 2 + 1)
            push_row(0, i)
            push_row(1, i)

    def lower_column(k):
        i = y - 1 - k

        @pl.when(i + x > 0)
        def _():
            hear(2 * side + i * 2)

        hear(2 * side + i * 2 + 1)
        push_column(0, i)
        push_column(1, i)

    loop(0, x, lower_row)
    loop(0, y, lower_column)

    @pl.when((c == 1) & (me > 1))
    def _():
        hear(x * 2)
        push_row(0, x)
        push_row(1, x)

    members = side - 1
    steps = (members - 1) // 2
    sub_rows = rows // SUBS
    others = rows - local

    def sub_ref(chunk, sub):
        return qall.at[chunk, pl.ds(sub * sub_rows, sub_rows), :]

    def member(offset):
        return (g - 1 + 2 * members + offset) % members + 1

    def ring(direction, step, sub):
        sign = 1 - 2 * direction
        ref = sub_ref(member(-sign * (step - 1)), sub)
        return pltpu.make_async_remote_copy(
            src_ref=ref,
            dst_ref=ref,
            send_sem=ring_send.at[direction, step - 1, sub],
            recv_sem=ring_recv.at[direction, step - 1, sub],
            device_id=line(a, member(sign), c),
            device_id_type=MESH,
        )

    def ring_wait(direction, step, sub):
        ref = sub_ref(member((2 * direction - 1) * step), sub)
        pltpu.make_async_copy(ref, ref, ring_recv.at[direction, step - 1, sub]).wait()

    def wait_own_queries():
        own[0].wait()
        ref = qall.at[0, pl.ds(0, others), :]
        pltpu.make_async_copy(ref, ref, p1_recv.at[0]).wait()

    @pl.when(g > 0)
    def _():
        wait_own_queries()
        for step in range(1, steps + 2):
            for sub in range(SUBS):
                for direction in range(2):
                    if step > 1:
                        ring_wait(direction, step - 1, sub)
                    if step <= steps:
                        ring(direction, step, sub).start()

    @pl.when((y == 0) & (me > 0))
    def _():
        hear(0)

        @pl.when(x > 0)
        def _():
            hear(1)

        push_row(0, 0)
        push_row(1, 0)

    @pl.when((x == 0) & (y > 0))
    def _():
        hear(2 * side)

    def direct(chunk, to):
        return pltpu.make_async_remote_copy(
            src_ref=qall.at[chunk],
            dst_ref=qall.at[chunk],
            send_sem=direct_send.at[to],
            recv_sem=direct_recv.at[chunk],
            device_id=line(a, to, c),
            device_id_type=MESH,
        )

    @pl.when(g > 0)
    def _():
        direct(g, 0).start()

    far_first = sorted(range(1, side), key=lambda i: -min(i, side - i))

    @pl.when(g == 0)
    def _():
        wait_own_queries()
        for to in far_first:
            direct(0, to).start()

    for copy in own[1:]:
        copy.wait()
    ref = kv.at[:, pl.ds(0, others), :]
    pltpu.make_async_copy(ref, ref, p1_recv.at[1]).wait()

    step_a = pair * (1 + c * (side - 1))
    step_g = pair * (side - c * (side - 1))
    end0 = sizes[0]
    end1 = end0 + sizes[1]
    end2 = end1 + sizes[2]

    def patches(count, start, chunk):
        l = lax.broadcasted_iota(jnp.int32, (count, HEAD), 0) + start
        pos = (l // pair) * step_a + chunk * step_g + l % pair
        one, zero = jnp.int32(1), jnp.int32(0)
        return sum(jnp.where(pos >= end, one, zero) for end in (end0, end1, end2))

    def indicator(mask):
        return jnp.where(mask, 1.0, 0.0).astype(jnp.bfloat16)

    key_patch = patches(rows, 0, g)
    for p in range(PATCHES):
        cols = pl.ds(p * HEAD, HEAD)
        fresh, stale = indicator(key_patch <= p), indicator(key_patch > p)
        kcat[:, cols] = kv[0] * fresh + kv[2] * stale
        vcat[:, cols] = kv[1] * fresh + kv[3] * stale

    eye = lax.broadcasted_iota(jnp.int32, (HEAD, HEAD), 0) == lax.broadcasted_iota(jnp.int32, (HEAD, HEAD), 1)
    contract = (((1,), (1,)), ((), ()))
    def compute(chunk):
        q = qall[chunk]
        patch = patches(rows, 0, chunk)
        split = jnp.concatenate([q * indicator(patch == p) for p in range(PATCHES)], axis=1)
        s = lax.dot_general(split, kcat[...], contract, preferred_element_type=jnp.float32)
        m = jnp.max(s, axis=1, keepdims=True)
        w = jnp.exp2((s - m) * scale2)
        total = jnp.sum(w, axis=1, keepdims=True)
        o = jnp.dot(w.astype(jnp.bfloat16), vcat[...], preferred_element_type=jnp.float32)
        picked = o[:, :HEAD]
        for p in range(1, PATCHES):
            picked = jnp.where(patch == p, o[:, p * HEAD : (p + 1) * HEAD], picked)
        opart[chunk] = (picked / total).astype(jnp.bfloat16)
        lse = m * scale2 + jnp.log2(total)
        for k in range(rows // HEAD):
            block_lse = lse[k * HEAD : (k + 1) * HEAD, :]
            lpart[chunk, pl.ds(k, 1), :] = jnp.sum(jnp.where(eye, block_lse, 0.0), axis=0, keepdims=True)

    def part(kind, chunk, source):
        src, dst = ((opart, orecv), (lpart, lrecv))[kind]
        return pltpu.make_async_remote_copy(
            src_ref=src.at[chunk],
            dst_ref=dst.at[source],
            send_sem=part_send.at[kind, chunk],
            recv_sem=part_recv.at[kind, source],
            device_id=line(a, chunk, c),
            device_id_type=MESH,
        )

    def one_chunk(k):
        chunk = side - 1 - k

        @pl.when((g == 0) & (chunk > 0))
        def _():
            pltpu.make_async_copy(qall.at[chunk], qall.at[chunk], direct_recv.at[chunk]).wait()

        @pl.when((g > 0) & (chunk == 0))
        def _():
            pltpu.make_async_copy(qall.at[0], qall.at[0], direct_recv.at[0]).wait()

        compute(chunk)

        @pl.when(chunk != g)
        def _():
            part(0, chunk, g).start()
            part(1, chunk, g).start()

    loop(0, side, one_chunk)

    orecv[g] = opart[g]
    lrecv[g] = lpart[g]

    def part_arrived(source):
        @pl.when(source != g)
        def _():
            pltpu.make_async_copy(orecv.at[source], orecv.at[source], part_recv.at[0, source]).wait()
            pltpu.make_async_copy(lrecv.at[source], lrecv.at[source], part_recv.at[1, source]).wait()

    loop(0, side, part_arrived)
    lse = [lrecv[source] for source in range(side)]
    top = functools.reduce(jnp.maximum, lse)
    weights = [jnp.exp2(l - top) for l in lse]
    total = functools.reduce(jnp.add, weights)
    weights = [w / total for w in weights]
    for t in range(rows // HEAD):
        acc = jnp.zeros((HEAD, HEAD), jnp.float32)
        for source in range(side):
            w = jnp.sum(jnp.where(eye, weights[source][t : t + 1, :], 0.0), axis=1, keepdims=True)
            acc = acc + w * orecv[source, pl.ds(t * HEAD, HEAD), :].astype(jnp.float32)
        outst[pl.ds(t * HEAD, HEAD), :] = acc.astype(jnp.bfloat16)

    def home(a_to, core):
        pltpu.make_async_remote_copy(
            src_ref=outst.at[block(a_to * 2 + core), :],
            dst_ref=out.at[:, head_cols(own_head)],
            send_sem=p4_send,
            recv_sem=p4_recv,
            device_id=line(a_to, g, core),
            device_id_type=MESH,
        ).start()

    for j in far_first:
        for core in range(2):
            home((a + j) % side, core)
    home(a, 1 - c)
    out[:, head_cols(own_head)] = outst[own_row, :]

    ref = qall.at[0, pl.ds(0, others), :]
    pltpu.make_async_copy(ref, ref, p1_send.at[0]).wait()
    ref = kv.at[:, pl.ds(0, others), :]
    pltpu.make_async_copy(ref, ref, p1_send.at[1]).wait()

    @pl.when(g > 0)
    def _():
        for step in range(1, steps + 1):
            for sub in range(SUBS):
                for direction in range(2):
                    ring(direction, step, sub).wait_send()
        direct(g, 0).wait_send()

    @pl.when(g == 0)
    def _():
        for to in far_first:
            direct(0, to).wait_send()

    def part_left(chunk):
        @pl.when(chunk != g)
        def _():
            part(0, chunk, g).wait_send()
            part(1, chunk, g).wait_send()

    loop(0, side, part_left)
    ref = outst.at[pl.ds(0, others), :]
    pltpu.make_async_copy(ref, ref, p4_recv).wait()
    pltpu.make_async_copy(ref, ref, p4_send).wait()


def shards(queries, fresh_keys, fresh_values, stale_keys, stale_values, patch_sizes):
    local, columns = queries.shape
    chips = lax.axis_size("seq") // 2
    side = math.isqrt(chips)
    assert side * side == chips and columns == 2 * side * HEAD
    rows = 2 * side * local
    half = side // 2
    bf16, f32 = jnp.bfloat16, jnp.float32
    dma = pltpu.SemaphoreType.DMA
    return pl.pallas_call(
        functools.partial(kernel, side, local),
        out_shape=jax.ShapeDtypeStruct((local, columns), bf16),
        in_specs=[pl.BlockSpec(memory_space=pltpu.SMEM)] + [pl.BlockSpec(memory_space=pl.ANY)] * 5,
        out_specs=pl.BlockSpec(memory_space=pltpu.VMEM),
        scratch_shapes=[
            pltpu.VMEM((5, local, columns), bf16),
            pltpu.VMEM((side, rows, HEAD), bf16),
            pltpu.VMEM((4, rows, HEAD), bf16),
            pltpu.VMEM((rows, PATCHES * HEAD), bf16),
            pltpu.VMEM((rows, PATCHES * HEAD), bf16),
            pltpu.VMEM((side, rows, HEAD), bf16),
            pltpu.VMEM((side, rows // HEAD, HEAD), f32),
            pltpu.VMEM((side, rows, HEAD), bf16),
            pltpu.VMEM((side, rows // HEAD, HEAD), f32),
            pltpu.VMEM((rows, HEAD), bf16),
            dma((5,)),
            dma((5,)),
            dma((2,)),
            dma((2,)),
            pltpu.SemaphoreType.REGULAR((4 * side,)),
            dma((2, half - 1, SUBS)),
            dma((2, half - 1, SUBS)),
            dma((side,)),
            dma((side,)),
            dma((2, side)),
            dma((2, side)),
            dma,
            dma,
        ],
        compiler_params=pltpu.CompilerParams(collective_id=0, has_side_effects=True),
    )(patch_sizes, queries, fresh_keys, fresh_values, stale_keys, stale_values)


def solution(mesh):
    in_specs = (
        P(("groups", "seq"), None),
        P(("groups", "seq"), None),
        P(("groups", "seq"), None),
        P(("groups", "seq"), None),
        P(("groups", "seq"), None),
        P("groups"),
    )
    out_specs = P(("groups", "seq"), None)
    return jax.shard_map(shards, mesh=mesh, in_specs=in_specs, out_specs=out_specs, check_vma=False)
```

```python
import functools
import math

import jax
import jax.numpy as jnp
from jax import lax
from jax.experimental import pallas as pl
from jax.experimental.pallas import tpu as pltpu
from jax.sharding import PartitionSpec as P

HEAD = 128
SUBS = 4
PATCHES = 4
MESH = pl.DeviceIdType.MESH


def kernel(
    side,
    local,
    sizes,
    q_in,
    fk_in,
    fv_in,
    sk_in,
    sv_in,
    out,
    stage,
    qall,
    kv,
    kcat,
    vcat,
    opart,
    lpart,
    orecv,
    lrecv,
    outst,
    load_sem,
    self_sem,
    p1_send,
    p1_recv,
    ready,
    ring_send,
    ring_recv,
    part_send,
    part_recv,
    p4_send,
    p4_recv,
):
    group = lax.axis_index("groups")
    me = lax.axis_index("seq")
    c = me % 2
    x = (me // 2) % side
    y = me // 2 // side
    a = x * (1 - c) + y * c
    g = y * (1 - c) + x * c
    rows = 2 * side * local
    half = side // 2
    pair = 2 * local
    scale2 = (HEAD**-0.5) * math.log2(math.e)

    def at(cx, cy, core):
        return (group, (cy * side + cx) * 2 + core)

    def line(a_to, g_to, core):
        return at(a_to * (1 - c) + g_to * c, g_to * (1 - c) + a_to * c, core)

    def head_cols(head):
        return pl.ds(pl.multiple_of(head * HEAD, HEAD), HEAD)

    inputs = (q_in, fk_in, fv_in, sk_in, sv_in)
    loads = [pltpu.make_async_copy(ref, stage.at[i], load_sem.at[i]) for i, ref in enumerate(inputs)]
    for copy in loads:
        copy.start()

    def block(index):
        return pl.ds(pl.multiple_of(index * local, local), local)

    def signal(semaphore, device):
        pl.semaphore_signal(semaphore, inc=1, device_id=device, device_id_type=MESH)

    def loop(first, last, body):
        def step(i, carry):
            body(i)
            return carry

        lax.fori_loop(first, last, step, 0)

    barrier = pltpu.get_barrier_semaphore()

    def greet_row(i):
        signal(barrier, at(i, y, 0))
        signal(barrier, at(i, y, 1))

    def greet_column(i):
        signal(barrier, at(x, i, 0))
        signal(barrier, at(x, i, 1))

    loop(0, x, greet_row)
    loop(0, y, greet_column)

    @pl.when(c == 1)
    def _():
        signal(barrier, at(x, y, 0))

    own_row = block(a * 2 + c)
    own_head = c * side + a
    own = []
    for i, ref in enumerate(inputs):
        dst = qall.at[g, own_row, :] if i == 0 else kv.at[i - 1, own_row, :]
        own.append(pltpu.make_async_copy(ref.at[:, head_cols(own_head)], dst, self_sem.at[i]))
        own[-1].start()

    higher = 2 * (side - 1 - x) + 2 * (side - 1 - y) + (1 - c)

    @pl.when(higher > 0)
    def _():
        pl.semaphore_wait(barrier, higher)

    def ready_row(i):
        signal(ready.at[x * 2 + c], at(i, y, 0))
        signal(ready.at[x * 2 + c], at(i, y, 1))

    def ready_column(i):
        signal(ready.at[2 * side + y * 2 + c], at(x, i, 0))
        signal(ready.at[2 * side + y * 2 + c], at(x, i, 1))

    loop(x + 1, side, ready_row)
    loop(y + 1, side, ready_column)

    @pl.when(c == 0)
    def _():
        signal(ready.at[x * 2], at(x, y, 1))

    row_x, row_y = block(x * 2 + c), block(y * 2 + c)

    def push(which, device, head, slot, row):
        if which == 0:
            src, dst = stage.at[0, :, head_cols(head)], qall.at[slot, row, :]
        else:
            src, dst = stage.at[pl.ds(1, 4), :, head_cols(head)], kv.at[:, row, :]
        pltpu.make_async_remote_copy(
            src_ref=src,
            dst_ref=dst,
            send_sem=p1_send.at[which],
            recv_sem=p1_recv.at[which],
            device_id=device,
            device_id_type=MESH,
        ).start()

    def push_row(which, i):
        push(which, at(i, y, 0), i, y, row_x)

    def push_column(which, i):
        push(which, at(x, i, 1), side + i, x, row_y)

    for which in range(2):
        for copy in loads[:1] if which == 0 else loads[1:]:
            copy.wait()
        loop(x + 1, side, functools.partial(push_row, which))
        loop(y + 1, side, functools.partial(push_column, which))

        @pl.when(c == 0)
        def _():
            push_column(which, y)

    def hear(index):
        pl.semaphore_wait(ready.at[index], 1)

    @pl.when(c == 1)
    def _():
        hear(x * 2)
        push_row(0, x)
        push_row(1, x)

    def lower_row(k):
        i = x - 1 - k
        hear(i * 2 + 1)
        hear(i * 2)
        push_row(0, i)
        push_row(1, i)

    def lower_column(k):
        i = y - 1 - k
        hear(2 * side + i * 2 + 1)
        push_column(0, i)
        push_column(1, i)
        hear(2 * side + i * 2)

    loop(0, x, lower_row)
    loop(0, y, lower_column)

    others = rows - local
    near_first = sorted(range(1, side), key=lambda i: min(i, side - i))

    def spread(delta, back=0, piece=None):
        chunk = (g + side - back) % side
        far = (delta + back) % side
        n = rows if piece is None else rows // 2
        ref = qall.at[chunk, pl.ds(0 if piece is None else piece * n, n), :]
        slot = far if piece != 1 else 0
        return pltpu.make_async_remote_copy(
            src_ref=ref,
            dst_ref=ref,
            send_sem=ring_send.at[slot],
            recv_sem=ring_recv.at[slot],
            device_id=line(a, (g + delta) % side, c),
            device_id_type=MESH,
        )

    def arrived(delta, piece=None):
        chunk = (g + side - delta) % side
        n = rows if piece is None else rows // 2
        ref = qall.at[chunk, pl.ds(0 if piece is None else piece * n, n), :]
        pltpu.make_async_copy(ref, ref, ring_recv.at[delta if piece != 1 else 0]).wait()

    firsts = (1, side - 1, 2, side - 2)
    first_hops = [spread(delta) for delta in firsts]
    second_hops = {
        2: [spread(1, 2), spread(2, 2, 0)],
        side - 2: [spread(side - 1, side - 2), spread(side - 2, side - 2, 1)],
    }

    own[0].wait()
    ref = qall.at[0, pl.ds(0, others), :]
    pltpu.make_async_copy(ref, ref, p1_recv.at[0]).wait()
    for copy in first_hops:
        copy.start()

    for copy in own[1:]:
        copy.wait()
    ref = kv.at[:, pl.ds(0, others), :]
    pltpu.make_async_copy(ref, ref, p1_recv.at[1]).wait()

    step_a = pair * (1 + c * (side - 1))
    step_g = pair * (side - c * (side - 1))
    end0 = sizes[0]
    end1 = end0 + sizes[1]
    end2 = end1 + sizes[2]

    def patches(count, start, chunk):
        l = lax.broadcasted_iota(jnp.int32, (count, HEAD), 0) + start
        pos = (l // pair) * step_a + chunk * step_g + l % pair
        one, zero = jnp.int32(1), jnp.int32(0)
        return sum(jnp.where(pos >= end, one, zero) for end in (end0, end1, end2))

    def indicator(mask):
        return jnp.where(mask, 1.0, 0.0).astype(jnp.bfloat16)

    key_patch = patches(rows, 0, g)
    for p in range(PATCHES):
        cols = pl.ds(p * HEAD, HEAD)
        fresh, stale = indicator(key_patch <= p), indicator(key_patch > p)
        kcat[:, cols] = kv[0] * fresh + kv[2] * stale
        vcat[:, cols] = kv[1] * fresh + kv[3] * stale

    eye = lax.broadcasted_iota(jnp.int32, (HEAD, HEAD), 0) == lax.broadcasted_iota(jnp.int32, (HEAD, HEAD), 1)
    contract = (((1,), (1,)), ((), ()))
    def compute(chunk):
        q = qall[chunk]
        patch = patches(rows, 0, chunk)
        split = jnp.concatenate([q * indicator(patch == p) for p in range(PATCHES)], axis=1)
        s = lax.dot_general(split, kcat[...], contract, preferred_element_type=jnp.float32)
        m = jnp.max(s, axis=1, keepdims=True)
        w = jnp.exp2((s - m) * scale2)
        total = jnp.sum(w, axis=1, keepdims=True)
        o = jnp.dot(w.astype(jnp.bfloat16), vcat[...], preferred_element_type=jnp.float32)
        picked = o[:, :HEAD]
        for p in range(1, PATCHES):
            picked = jnp.where(patch == p, o[:, p * HEAD : (p + 1) * HEAD], picked)
        opart[chunk] = (picked / total).astype(jnp.bfloat16)
        lse = m * scale2 + jnp.log2(total)
        for k in range(rows // HEAD):
            block_lse = lse[k * HEAD : (k + 1) * HEAD, :]
            lpart[chunk, pl.ds(k, 1), :] = jnp.sum(jnp.where(eye, block_lse, 0.0), axis=0, keepdims=True)

    def part(kind, chunk, source):
        src, dst = ((opart, orecv), (lpart, lrecv))[kind]
        return pltpu.make_async_remote_copy(
            src_ref=src.at[chunk],
            dst_ref=dst.at[source],
            send_sem=part_send.at[kind, chunk],
            recv_sem=part_recv.at[kind, source],
            device_id=line(a, chunk, c),
            device_id_type=MESH,
        )

    def do_part(delta):
        chunk = (g + side - delta) % side
        compute(chunk)
        part(0, chunk, g).start()
        part(1, chunk, g).start()

    def pass_on(delta):
        arrived(delta)
        for copy in second_hops[delta]:
            copy.start()

    compute(g)
    for delta in (1, side - 1):
        arrived(delta)
        do_part(delta)
    pass_on(2)
    pass_on(side - 2)
    do_part(2)
    do_part(side - 2)
    for delta in (3, side - 3):
        arrived(delta)
        do_part(delta)
    arrived(half, 0)
    arrived(half, 1)
    do_part(half)

    orecv[g] = opart[g]
    lrecv[g] = lpart[g]

    def part_arrived(source):
        @pl.when(source != g)
        def _():
            pltpu.make_async_copy(orecv.at[source], orecv.at[source], part_recv.at[0, source]).wait()
            pltpu.make_async_copy(lrecv.at[source], lrecv.at[source], part_recv.at[1, source]).wait()

    loop(0, side, part_arrived)
    lse = [lrecv[source] for source in range(side)]
    top = functools.reduce(jnp.maximum, lse)
    weights = [jnp.exp2(l - top) for l in lse]
    total = functools.reduce(jnp.add, weights)
    weights = [w / total for w in weights]
    for t in range(rows // HEAD):
        acc = jnp.zeros((HEAD, HEAD), jnp.float32)
        for source in range(side):
            w = jnp.sum(jnp.where(eye, weights[source][t : t + 1, :], 0.0), axis=1, keepdims=True)
            acc = acc + w * orecv[source, pl.ds(t * HEAD, HEAD), :].astype(jnp.float32)
        outst[pl.ds(t * HEAD, HEAD), :] = acc.astype(jnp.bfloat16)

    def home(a_to, core):
        pltpu.make_async_remote_copy(
            src_ref=outst.at[block(a_to * 2 + core), :],
            dst_ref=out.at[:, head_cols(own_head)],
            send_sem=p4_send,
            recv_sem=p4_recv,
            device_id=line(a_to, g, core),
            device_id_type=MESH,
        ).start()

    for j in sorted(range(1, side), key=lambda i: min(i, side - i)):
        for core in range(2):
            home((a + j) % side, core)
    home(a, 1 - c)
    out[:, head_cols(own_head)] = outst[own_row, :]

    ref = qall.at[0, pl.ds(0, others), :]
    pltpu.make_async_copy(ref, ref, p1_send.at[0]).wait()
    ref = kv.at[:, pl.ds(0, others), :]
    pltpu.make_async_copy(ref, ref, p1_send.at[1]).wait()

    for copy in first_hops + second_hops[2] + second_hops[side - 2]:
        copy.wait_send()

    def part_left(chunk):
        @pl.when(chunk != g)
        def _():
            part(0, chunk, g).wait_send()
            part(1, chunk, g).wait_send()

    loop(0, side, part_left)
    ref = outst.at[pl.ds(0, others), :]
    pltpu.make_async_copy(ref, ref, p4_recv).wait()
    pltpu.make_async_copy(ref, ref, p4_send).wait()


def shards(queries, fresh_keys, fresh_values, stale_keys, stale_values, patch_sizes):
    local, columns = queries.shape
    chips = lax.axis_size("seq") // 2
    side = math.isqrt(chips)
    assert side * side == chips and columns == 2 * side * HEAD
    rows = 2 * side * local
    half = side // 2
    bf16, f32 = jnp.bfloat16, jnp.float32
    dma = pltpu.SemaphoreType.DMA
    return pl.pallas_call(
        functools.partial(kernel, side, local),
        out_shape=jax.ShapeDtypeStruct((local, columns), bf16),
        in_specs=[pl.BlockSpec(memory_space=pltpu.SMEM)] + [pl.BlockSpec(memory_space=pl.ANY)] * 5,
        out_specs=pl.BlockSpec(memory_space=pltpu.VMEM),
        scratch_shapes=[
            pltpu.VMEM((5, local, columns), bf16),
            pltpu.VMEM((side, rows, HEAD), bf16),
            pltpu.VMEM((4, rows, HEAD), bf16),
            pltpu.VMEM((rows, PATCHES * HEAD), bf16),
            pltpu.VMEM((rows, PATCHES * HEAD), bf16),
            pltpu.VMEM((side, rows, HEAD), bf16),
            pltpu.VMEM((side, rows // HEAD, HEAD), f32),
            pltpu.VMEM((side, rows, HEAD), bf16),
            pltpu.VMEM((side, rows // HEAD, HEAD), f32),
            pltpu.VMEM((rows, HEAD), bf16),
            dma((5,)),
            dma((5,)),
            dma((2,)),
            dma((2,)),
            pltpu.SemaphoreType.REGULAR((4 * side,)),
            dma((side,)),
            dma((side,)),
            dma((2, side)),
            dma((2, side)),
            dma,
            dma,
        ],
        compiler_params=pltpu.CompilerParams(collective_id=0, has_side_effects=True),
    )(patch_sizes, queries, fresh_keys, fresh_values, stale_keys, stale_values)


def solution(mesh):
    in_specs = (
        P(("groups", "seq"), None),
        P(("groups", "seq"), None),
        P(("groups", "seq"), None),
        P(("groups", "seq"), None),
        P(("groups", "seq"), None),
        P("groups"),
    )
    out_specs = P(("groups", "seq"), None)
    return jax.shard_map(shards, mesh=mesh, in_specs=in_specs, out_specs=out_specs, check_vma=False)
```

```python
import functools
import math

import jax
import jax.numpy as jnp
from jax import lax
from jax.experimental import pallas as pl
from jax.experimental.pallas import tpu as pltpu
from jax.sharding import PartitionSpec as P

HEAD = 128
SUBS = 4
PATCHES = 4
MESH = pl.DeviceIdType.MESH


def kernel(
    side,
    local,
    sizes,
    q_in,
    fk_in,
    fv_in,
    sk_in,
    sv_in,
    out,
    stage,
    qall,
    kv,
    kcat,
    vcat,
    opart,
    lpart,
    orecv,
    lrecv,
    outst,
    load_sem,
    self_sem,
    p1_send,
    p1_recv,
    ready,
    ring_send,
    ring_recv,
    part_send,
    part_recv,
    p4_send,
    p4_recv,
):
    group = lax.axis_index("groups")
    me = lax.axis_index("seq")
    c = me % 2
    x = (me // 2) % side
    y = me // 2 // side
    a = x * (1 - c) + y * c
    g = y * (1 - c) + x * c
    rows = 2 * side * local
    half = side // 2
    pair = 2 * local
    scale2 = (HEAD**-0.5) * math.log2(math.e)

    def at(cx, cy, core):
        return (group, (cy * side + cx) * 2 + core)

    def line(a_to, g_to, core):
        return at(a_to * (1 - c) + g_to * c, g_to * (1 - c) + a_to * c, core)

    def head_cols(head):
        return pl.ds(pl.multiple_of(head * HEAD, HEAD), HEAD)

    inputs = (q_in, fk_in, fv_in, sk_in, sv_in)
    loads = [pltpu.make_async_copy(ref, stage.at[i], load_sem.at[i]) for i, ref in enumerate(inputs)]
    for copy in loads:
        copy.start()

    def block(index):
        return pl.ds(pl.multiple_of(index * local, local), local)

    def signal(semaphore, device):
        pl.semaphore_signal(semaphore, inc=1, device_id=device, device_id_type=MESH)

    def loop(first, last, body):
        def step(i, carry):
            body(i)
            return carry

        lax.fori_loop(first, last, step, 0)

    barrier = pltpu.get_barrier_semaphore()

    def greet_row(i):
        signal(barrier, at(i, y, 0))
        signal(barrier, at(i, y, 1))

    def greet_column(i):
        signal(barrier, at(x, i, 0))
        signal(barrier, at(x, i, 1))

    loop(0, x, greet_row)
    loop(0, y, greet_column)

    @pl.when(c == 1)
    def _():
        signal(barrier, at(x, y, 0))

    own_row = block(a * 2 + c)
    own_head = c * side + a
    own = []
    for i, ref in enumerate(inputs):
        dst = qall.at[g, own_row, :] if i == 0 else kv.at[i - 1, own_row, :]
        own.append(pltpu.make_async_copy(ref.at[:, head_cols(own_head)], dst, self_sem.at[i]))
        own[-1].start()

    higher = 2 * (side - 1 - x) + 2 * (side - 1 - y) + (1 - c)

    @pl.when(higher > 0)
    def _():
        pl.semaphore_wait(barrier, higher)

    def ready_row(i):
        signal(ready.at[x * 2 + c], at(i, y, 0))
        signal(ready.at[x * 2 + c], at(i, y, 1))

    def ready_column(i):
        signal(ready.at[2 * side + y * 2 + c], at(x, i, 0))
        signal(ready.at[2 * side + y * 2 + c], at(x, i, 1))

    loop(x + 1, side, ready_row)
    loop(y + 1, side, ready_column)

    @pl.when(c == 0)
    def _():
        signal(ready.at[x * 2], at(x, y, 1))

    row_x, row_y = block(x * 2 + c), block(y * 2 + c)

    def push(which, device, head, slot, row):
        if which == 0:
            src, dst = stage.at[0, :, head_cols(head)], qall.at[slot, row, :]
        else:
            src, dst = stage.at[pl.ds(1, 4), :, head_cols(head)], kv.at[:, row, :]
        pltpu.make_async_remote_copy(
            src_ref=src,
            dst_ref=dst,
            send_sem=p1_send.at[which],
            recv_sem=p1_recv.at[which],
            device_id=device,
            device_id_type=MESH,
        ).start()

    def push_row(which, i):
        push(which, at(i, y, 0), i, y, row_x)

    def push_column(which, i):
        push(which, at(x, i, 1), side + i, x, row_y)

    for which in range(2):
        for copy in loads[:1] if which == 0 else loads[1:]:
            copy.wait()
        loop(x + 1, side, functools.partial(push_row, which))
        loop(y + 1, side, functools.partial(push_column, which))

        @pl.when(c == 0)
        def _():
            push_column(which, y)

    def hear(index):
        pl.semaphore_wait(ready.at[index], 1)

    @pl.when(c == 1)
    def _():
        hear(x * 2)
        push_row(0, x)
        push_row(1, x)

    def lower_row(k):
        i = x - 1 - k
        hear(i * 2 + 1)
        hear(i * 2)
        push_row(0, i)
        push_row(1, i)

    def lower_column(k):
        i = y - 1 - k
        hear(2 * side + i * 2 + 1)
        push_column(0, i)
        push_column(1, i)
        hear(2 * side + i * 2)

    loop(0, x, lower_row)
    loop(0, y, lower_column)

    others = rows - local
    near_first = sorted(range(1, side), key=lambda i: min(i, side - i))

    def spread(delta, back=0, piece=None):
        chunk = (g + side - back) % side
        far = (delta + back) % side
        n = rows if piece is None else rows // 2
        ref = qall.at[chunk, pl.ds(0 if piece is None else piece * n, n), :]
        slot = far if piece != 1 else 0
        return pltpu.make_async_remote_copy(
            src_ref=ref,
            dst_ref=ref,
            send_sem=ring_send.at[slot],
            recv_sem=ring_recv.at[slot],
            device_id=line(a, (g + delta) % side, c),
            device_id_type=MESH,
        )

    def arrived(delta, piece=None):
        chunk = (g + side - delta) % side
        n = rows if piece is None else rows // 2
        ref = qall.at[chunk, pl.ds(0 if piece is None else piece * n, n), :]
        pltpu.make_async_copy(ref, ref, ring_recv.at[delta if piece != 1 else 0]).wait()

    firsts = (1, side - 1, 2, side - 2)
    first_hops = [spread(delta) for delta in firsts]
    second_hops = {
        2: [spread(1, 2), spread(2, 2, 0)],
        side - 2: [spread(side - 1, side - 2), spread(side - 2, side - 2, 1)],
    }

    own[0].wait()
    ref = qall.at[0, pl.ds(0, others), :]
    pltpu.make_async_copy(ref, ref, p1_recv.at[0]).wait()
    for copy in first_hops:
        copy.start()

    for copy in own[1:]:
        copy.wait()
    ref = kv.at[:, pl.ds(0, others), :]
    pltpu.make_async_copy(ref, ref, p1_recv.at[1]).wait()

    step_a = pair * (1 + c * (side - 1))
    step_g = pair * (side - c * (side - 1))
    end0 = sizes[0]
    end1 = end0 + sizes[1]
    end2 = end1 + sizes[2]

    def patches(count, start, chunk):
        l = lax.broadcasted_iota(jnp.int32, (count, HEAD), 0) + start
        pos = (l // pair) * step_a + chunk * step_g + l % pair
        one, zero = jnp.int32(1), jnp.int32(0)
        return sum(jnp.where(pos >= end, one, zero) for end in (end0, end1, end2))

    def indicator(mask):
        return jnp.where(mask, 1.0, 0.0).astype(jnp.bfloat16)

    key_patch = patches(rows, 0, g)
    for p in range(PATCHES):
        cols = pl.ds(p * HEAD, HEAD)
        fresh, stale = indicator(key_patch <= p), indicator(key_patch > p)
        kcat[:, cols] = kv[0] * fresh + kv[2] * stale
        vcat[:, cols] = kv[1] * fresh + kv[3] * stale

    eye = lax.broadcasted_iota(jnp.int32, (HEAD, HEAD), 0) == lax.broadcasted_iota(jnp.int32, (HEAD, HEAD), 1)
    contract = (((1,), (1,)), ((), ()))
    def compute(chunk, first=0, count=rows):
        q = qall[chunk, pl.ds(first, count), :]
        patch = patches(count, first, chunk)
        split = jnp.concatenate([q * indicator(patch == p) for p in range(PATCHES)], axis=1)
        s = lax.dot_general(split, kcat[...], contract, preferred_element_type=jnp.float32)
        m = jnp.max(s, axis=1, keepdims=True)
        w = jnp.exp2((s - m) * scale2)
        total = jnp.sum(w, axis=1, keepdims=True)
        o = jnp.dot(w.astype(jnp.bfloat16), vcat[...], preferred_element_type=jnp.float32)
        picked = o[:, :HEAD]
        for p in range(1, PATCHES):
            picked = jnp.where(patch == p, o[:, p * HEAD : (p + 1) * HEAD], picked)
        opart[chunk, pl.ds(first, count), :] = (picked / total).astype(jnp.bfloat16)
        lse = m * scale2 + jnp.log2(total)
        for k in range(count // HEAD):
            block_lse = lse[k * HEAD : (k + 1) * HEAD, :]
            lpart[chunk, pl.ds(first // HEAD + k, 1), :] = jnp.sum(jnp.where(eye, block_lse, 0.0), axis=0, keepdims=True)

    def part(kind, chunk, source, piece=None):
        src, dst = ((opart, orecv), (lpart, lrecv))[kind]
        n = src.shape[1]
        cut = pl.ds(0, n) if piece is None else pl.ds(piece * (n // 2), n // 2)
        extra = piece == 1
        return pltpu.make_async_remote_copy(
            src_ref=src.at[chunk, cut],
            dst_ref=dst.at[source, cut],
            send_sem=part_send.at[kind, side if extra else chunk],
            recv_sem=part_recv.at[kind, side if extra else source],
            device_id=line(a, chunk, c),
            device_id_type=MESH,
        )

    def do_part(delta):
        chunk = (g + side - delta) % side
        compute(chunk)
        part(0, chunk, g).start()
        part(1, chunk, g).start()

    def pass_on(delta):
        arrived(delta)
        for copy in second_hops[delta]:
            copy.start()

    compute(g)
    for delta in (1, side - 1):
        arrived(delta)
        do_part(delta)
    pass_on(2)
    pass_on(side - 2)
    do_part(2)
    do_part(side - 2)
    for delta in (3, side - 3):
        arrived(delta)
        do_part(delta)
    opposite = (g + half) % side
    halves = [(kind, piece) for piece in range(2) for kind in range(2)]
    for piece in range(2):
        arrived(half, piece)
        compute(opposite, piece * (rows // 2), rows // 2)
        for kind in range(2):
            part(kind, opposite, g, piece).start()

    orecv[g] = opart[g]
    lrecv[g] = lpart[g]

    def part_arrived(delta):
        source = (g + delta) % side

        @pl.when(delta != half)
        def _():
            pltpu.make_async_copy(orecv.at[source], orecv.at[source], part_recv.at[0, source]).wait()
            pltpu.make_async_copy(lrecv.at[source], lrecv.at[source], part_recv.at[1, source]).wait()

    def piece_arrived(piece):
        for kind, ref in enumerate((orecv, lrecv)):
            n = ref.shape[1] // 2
            cut = ref.at[opposite, pl.ds(piece * n, n)]
            pltpu.make_async_copy(cut, cut, part_recv.at[kind, side if piece else opposite]).wait()

    def home(a_to, core):
        pltpu.make_async_remote_copy(
            src_ref=outst.at[block(a_to * 2 + core), :],
            dst_ref=out.at[:, head_cols(own_head)],
            send_sem=p4_send,
            recv_sem=p4_recv,
            device_id=line(a_to, g, core),
            device_id_type=MESH,
        ).start()

    def finish(piece):
        n = rows // HEAD // 2
        lse = [lrecv[source, pl.ds(piece * n, n)] for source in range(side)]
        top = functools.reduce(jnp.maximum, lse)
        weights = [jnp.exp2(l - top) for l in lse]
        total = functools.reduce(jnp.add, weights)
        weights = [w / total for w in weights]
        for k in range(n):
            tile = pl.ds((piece * n + k) * HEAD, HEAD)
            acc = jnp.zeros((HEAD, HEAD), jnp.float32)
            for source in range(side):
                w = jnp.sum(jnp.where(eye, weights[source][k : k + 1, :], 0.0), axis=1, keepdims=True)
                acc = acc + w * orecv[source, tile, :].astype(jnp.float32)
            outst[tile, :] = acc.astype(jnp.bfloat16)
        for j in near_first:
            to = (a + j) % side

            @pl.when(to // half == piece)
            def _():
                home(to, 0)
                home(to, 1)

        @pl.when(a // half == piece)
        def _():
            home(a, 1 - c)
            out[:, head_cols(own_head)] = outst[own_row, :]

    loop(1, side, part_arrived)
    for piece in range(2):
        piece_arrived(piece)
        finish(piece)

    ref = qall.at[0, pl.ds(0, others), :]
    pltpu.make_async_copy(ref, ref, p1_send.at[0]).wait()
    ref = kv.at[:, pl.ds(0, others), :]
    pltpu.make_async_copy(ref, ref, p1_send.at[1]).wait()

    for copy in first_hops + second_hops[2] + second_hops[side - 2]:
        copy.wait_send()

    def part_left(delta):
        chunk = (g + delta) % side

        @pl.when(delta != half)
        def _():
            part(0, chunk, g).wait_send()
            part(1, chunk, g).wait_send()

    loop(1, side, part_left)
    for kind, piece in halves:
        part(kind, opposite, g, piece).wait_send()
    ref = outst.at[pl.ds(0, others), :]
    pltpu.make_async_copy(ref, ref, p4_recv).wait()
    pltpu.make_async_copy(ref, ref, p4_send).wait()


def shards(queries, fresh_keys, fresh_values, stale_keys, stale_values, patch_sizes):
    local, columns = queries.shape
    chips = lax.axis_size("seq") // 2
    side = math.isqrt(chips)
    assert side * side == chips and columns == 2 * side * HEAD
    rows = 2 * side * local
    half = side // 2
    bf16, f32 = jnp.bfloat16, jnp.float32
    dma = pltpu.SemaphoreType.DMA
    return pl.pallas_call(
        functools.partial(kernel, side, local),
        out_shape=jax.ShapeDtypeStruct((local, columns), bf16),
        in_specs=[pl.BlockSpec(memory_space=pltpu.SMEM)] + [pl.BlockSpec(memory_space=pl.ANY)] * 5,
        out_specs=pl.BlockSpec(memory_space=pltpu.VMEM),
        scratch_shapes=[
            pltpu.VMEM((5, local, columns), bf16),
            pltpu.VMEM((side, rows, HEAD), bf16),
            pltpu.VMEM((4, rows, HEAD), bf16),
            pltpu.VMEM((rows, PATCHES * HEAD), bf16),
            pltpu.VMEM((rows, PATCHES * HEAD), bf16),
            pltpu.VMEM((side, rows, HEAD), bf16),
            pltpu.VMEM((side, rows // HEAD, HEAD), f32),
            pltpu.VMEM((side, rows, HEAD), bf16),
            pltpu.VMEM((side, rows // HEAD, HEAD), f32),
            pltpu.VMEM((rows, HEAD), bf16),
            dma((5,)),
            dma((5,)),
            dma((2,)),
            dma((2,)),
            pltpu.SemaphoreType.REGULAR((4 * side,)),
            dma((side,)),
            dma((side,)),
            dma((2, side + 1)),
            dma((2, side + 1)),
            dma,
            dma,
        ],
        compiler_params=pltpu.CompilerParams(collective_id=0, has_side_effects=True),
    )(patch_sizes, queries, fresh_keys, fresh_values, stale_keys, stale_values)


def solution(mesh):
    in_specs = (
        P(("groups", "seq"), None),
        P(("groups", "seq"), None),
        P(("groups", "seq"), None),
        P(("groups", "seq"), None),
        P(("groups", "seq"), None),
        P("groups"),
    )
    out_specs = P(("groups", "seq"), None)
    return jax.shard_map(shards, mesh=mesh, in_specs=in_specs, out_specs=out_specs, check_vma=False)
```

```python
import functools
import math

import jax
import jax.numpy as jnp
from jax import lax
from jax.experimental import pallas as pl
from jax.experimental.pallas import tpu as pltpu
from jax.sharding import PartitionSpec as P

HEAD = 128
SUBS = 4
PATCHES = 4
MESH = pl.DeviceIdType.MESH


def kernel(
    side,
    local,
    sizes,
    q_in,
    fk_in,
    fv_in,
    sk_in,
    sv_in,
    out,
    stage,
    qall,
    kv,
    kcat,
    vcat,
    opart,
    lpart,
    orecv,
    lrecv,
    outst,
    load_sem,
    self_sem,
    p1_send,
    p1_recv,
    ready,
    ring_send,
    ring_recv,
    part_send,
    part_recv,
    p4_send,
    p4_recv,
):
    group = lax.axis_index("groups")
    me = lax.axis_index("seq")
    c = me % 2
    x = (me // 2) % side
    y = me // 2 // side
    a = x * (1 - c) + y * c
    g = y * (1 - c) + x * c
    rows = 2 * side * local
    half = side // 2
    pair = 2 * local
    scale2 = (HEAD**-0.5) * math.log2(math.e)

    def at(cx, cy, core):
        return (group, (cy * side + cx) * 2 + core)

    def line(a_to, g_to, core):
        return at(a_to * (1 - c) + g_to * c, g_to * (1 - c) + a_to * c, core)

    def head_cols(head):
        return pl.ds(pl.multiple_of(head * HEAD, HEAD), HEAD)

    inputs = (q_in, fk_in, fv_in, sk_in, sv_in)
    loads = [pltpu.make_async_copy(ref, stage.at[i], load_sem.at[i]) for i, ref in enumerate(inputs)]
    for copy in loads:
        copy.start()

    def block(index):
        return pl.ds(pl.multiple_of(index * local, local), local)

    def signal(semaphore, device):
        pl.semaphore_signal(semaphore, inc=1, device_id=device, device_id_type=MESH)

    def loop(first, last, body):
        def step(i, carry):
            body(i)
            return carry

        lax.fori_loop(first, last, step, 0)

    barrier = pltpu.get_barrier_semaphore()

    def greet_row(i):
        signal(barrier, at(i, y, 0))
        signal(barrier, at(i, y, 1))

    def greet_column(i):
        signal(barrier, at(x, i, 0))
        signal(barrier, at(x, i, 1))

    loop(0, x, greet_row)
    loop(0, y, greet_column)

    @pl.when(c == 1)
    def _():
        signal(barrier, at(x, y, 0))

    higher = 2 * (side - 1 - x) + 2 * (side - 1 - y) + (1 - c)

    @pl.when(higher > 0)
    def _():
        pl.semaphore_wait(barrier, higher)

    def ready_row(i):
        signal(ready.at[x * 2 + c], at(i, y, 0))
        signal(ready.at[x * 2 + c], at(i, y, 1))

    def ready_column(i):
        signal(ready.at[2 * side + y * 2 + c], at(x, i, 0))
        signal(ready.at[2 * side + y * 2 + c], at(x, i, 1))

    loop(x + 1, side, ready_row)
    loop(y + 1, side, ready_column)

    @pl.when(c == 0)
    def _():
        signal(ready.at[x * 2], at(x, y, 1))

    own_row = block(a * 2 + c)
    own_head = c * side + a
    own = []
    for i, ref in enumerate(inputs):
        dst = qall.at[g, own_row, :] if i == 0 else kv.at[i - 1, own_row, :]
        own.append(pltpu.make_async_copy(ref.at[:, head_cols(own_head)], dst, self_sem.at[i]))
        own[-1].start()

    row_x, row_y = block(x * 2 + c), block(y * 2 + c)

    def push(which, device, head, slot, row):
        if which == 0:
            src, dst = stage.at[0, :, head_cols(head)], qall.at[slot, row, :]
        else:
            src, dst = stage.at[pl.ds(1, 4), :, head_cols(head)], kv.at[:, row, :]
        pltpu.make_async_remote_copy(
            src_ref=src,
            dst_ref=dst,
            send_sem=p1_send.at[which],
            recv_sem=p1_recv.at[which],
            device_id=device,
            device_id_type=MESH,
        ).start()

    def push_row(which, i):
        push(which, at(i, y, 0), i, y, row_x)

    def push_column(which, i):
        push(which, at(x, i, 1), side + i, x, row_y)

    for which in range(2):
        for copy in loads[:1] if which == 0 else loads[1:]:
            copy.wait()
        loop(x + 1, side, functools.partial(push_row, which))
        loop(y + 1, side, functools.partial(push_column, which))

        @pl.when(c == 0)
        def _():
            push_column(which, y)

    def hear(index):
        pl.semaphore_wait(ready.at[index], 1)

    @pl.when(c == 1)
    def _():
        hear(x * 2)
        push_row(0, x)
        push_row(1, x)

    def lower_row(k):
        i = x - 1 - k
        hear(i * 2 + 1)
        hear(i * 2)
        push_row(0, i)
        push_row(1, i)

    def lower_column(k):
        i = y - 1 - k
        hear(2 * side + i * 2 + 1)
        push_column(0, i)
        push_column(1, i)
        hear(2 * side + i * 2)

    loop(0, x, lower_row)
    loop(0, y, lower_column)

    others = rows - local
    near_first = sorted(range(1, side), key=lambda i: min(i, side - i))

    def spread(delta, back=0, piece=None):
        chunk = (g + side - back) % side
        far = (delta + back) % side
        n = rows if piece is None else rows // 2
        ref = qall.at[chunk, pl.ds(0 if piece is None else piece * n, n), :]
        slot = far if piece != 1 else 0
        return pltpu.make_async_remote_copy(
            src_ref=ref,
            dst_ref=ref,
            send_sem=ring_send.at[slot],
            recv_sem=ring_recv.at[slot],
            device_id=line(a, (g + delta) % side, c),
            device_id_type=MESH,
        )

    def arrived(delta, piece=None):
        chunk = (g + side - delta) % side
        n = rows if piece is None else rows // 2
        ref = qall.at[chunk, pl.ds(0 if piece is None else piece * n, n), :]
        pltpu.make_async_copy(ref, ref, ring_recv.at[delta if piece != 1 else 0]).wait()

    firsts = (1, side - 1, 2, side - 2)
    first_hops = [spread(delta) for delta in firsts]
    second_hops = {
        2: [spread(1, 2), spread(2, 2, 0)],
        side - 2: [spread(side - 1, side - 2), spread(side - 2, side - 2, 1)],
    }

    own[0].wait()
    ref = qall.at[0, pl.ds(0, others), :]
    pltpu.make_async_copy(ref, ref, p1_recv.at[0]).wait()
    for copy in first_hops:
        copy.start()

    for copy in own[1:]:
        copy.wait()
    ref = kv.at[:, pl.ds(0, others), :]
    pltpu.make_async_copy(ref, ref, p1_recv.at[1]).wait()

    step_a = pair * (1 + c * (side - 1))
    step_g = pair * (side - c * (side - 1))
    end0 = sizes[0]
    end1 = end0 + sizes[1]
    end2 = end1 + sizes[2]

    def patches(count, start, chunk):
        l = lax.broadcasted_iota(jnp.int32, (count, HEAD), 0) + start
        pos = (l // pair) * step_a + chunk * step_g + l % pair
        one, zero = jnp.int32(1), jnp.int32(0)
        return sum(jnp.where(pos >= end, one, zero) for end in (end0, end1, end2))

    def indicator(mask):
        return jnp.where(mask, 1.0, 0.0).astype(jnp.bfloat16)

    key_patch = patches(rows, 0, g)
    for p in range(PATCHES):
        cols = pl.ds(p * HEAD, HEAD)
        fresh, stale = indicator(key_patch <= p), indicator(key_patch > p)
        kcat[:, cols] = kv[0] * fresh + kv[2] * stale
        vcat[:, cols] = kv[1] * fresh + kv[3] * stale

    eye = lax.broadcasted_iota(jnp.int32, (HEAD, HEAD), 0) == lax.broadcasted_iota(jnp.int32, (HEAD, HEAD), 1)
    contract = (((1,), (1,)), ((), ()))
    def compute(chunk, first=0, count=rows):
        q = qall[chunk, pl.ds(first, count), :]
        patch = patches(count, first, chunk)
        split = jnp.concatenate([q * indicator(patch == p) for p in range(PATCHES)], axis=1)
        s = lax.dot_general(split, kcat[...], contract, preferred_element_type=jnp.float32)
        m = jnp.max(s, axis=1, keepdims=True)
        w = jnp.exp2((s - m) * scale2)
        total = jnp.sum(w, axis=1, keepdims=True)
        o = jnp.dot(w.astype(jnp.bfloat16), vcat[...], preferred_element_type=jnp.float32)
        picked = o[:, :HEAD]
        for p in range(1, PATCHES):
            picked = jnp.where(patch == p, o[:, p * HEAD : (p + 1) * HEAD], picked)
        opart[chunk, pl.ds(first, count), :] = (picked / total).astype(jnp.bfloat16)
        lse = m * scale2 + jnp.log2(total)
        for k in range(count // HEAD):
            block_lse = lse[k * HEAD : (k + 1) * HEAD, :]
            lpart[chunk, pl.ds(first // HEAD + k, 1), :] = jnp.sum(jnp.where(eye, block_lse, 0.0), axis=0, keepdims=True)

    def part(kind, chunk, source, piece=None):
        src, dst = ((opart, orecv), (lpart, lrecv))[kind]
        n = src.shape[1]
        cut = pl.ds(0, n) if piece is None else pl.ds(piece * (n // 2), n // 2)
        extra = piece == 1
        return pltpu.make_async_remote_copy(
            src_ref=src.at[chunk, cut],
            dst_ref=dst.at[source, cut],
            send_sem=part_send.at[kind, side if extra else chunk],
            recv_sem=part_recv.at[kind, side if extra else source],
            device_id=line(a, chunk, c),
            device_id_type=MESH,
        )

    def do_part(delta):
        chunk = (g + side - delta) % side
        compute(chunk)
        part(0, chunk, g).start()
        part(1, chunk, g).start()

    def pass_on(delta):
        arrived(delta)
        for copy in second_hops[delta]:
            copy.start()

    compute(g)
    for delta in (1, side - 1):
        arrived(delta)
        do_part(delta)
    pass_on(2)
    pass_on(side - 2)
    do_part(2)
    do_part(side - 2)
    for delta in (3, side - 3):
        arrived(delta)
        do_part(delta)
    opposite = (g + half) % side
    halves = [(kind, piece) for piece in range(2) for kind in range(2)]
    for piece in range(2):
        arrived(half, piece)
        compute(opposite, piece * (rows // 2), rows // 2)
        for kind in range(2):
            part(kind, opposite, g, piece).start()

    orecv[g] = opart[g]
    lrecv[g] = lpart[g]

    def part_arrived(delta):
        source = (g + delta) % side

        @pl.when(delta != half)
        def _():
            pltpu.make_async_copy(orecv.at[source], orecv.at[source], part_recv.at[0, source]).wait()
            pltpu.make_async_copy(lrecv.at[source], lrecv.at[source], part_recv.at[1, source]).wait()

    def piece_arrived(piece):
        for kind, ref in enumerate((orecv, lrecv)):
            n = ref.shape[1] // 2
            cut = ref.at[opposite, pl.ds(piece * n, n)]
            pltpu.make_async_copy(cut, cut, part_recv.at[kind, side if piece else opposite]).wait()

    def home(a_to, core):
        pltpu.make_async_remote_copy(
            src_ref=outst.at[block(a_to * 2 + core), :],
            dst_ref=out.at[:, head_cols(own_head)],
            send_sem=p4_send,
            recv_sem=p4_recv,
            device_id=line(a_to, g, core),
            device_id_type=MESH,
        ).start()

    def finish(piece):
        n = rows // HEAD // 2
        lse = [lrecv[source, pl.ds(piece * n, n)] for source in range(side)]
        top = functools.reduce(jnp.maximum, lse)
        weights = [jnp.exp2(l - top) for l in lse]
        total = functools.reduce(jnp.add, weights)
        weights = [w / total for w in weights]
        for k in range(n):
            tile = pl.ds((piece * n + k) * HEAD, HEAD)
            acc = jnp.zeros((HEAD, HEAD), jnp.float32)
            for source in range(side):
                w = jnp.sum(jnp.where(eye, weights[source][k : k + 1, :], 0.0), axis=1, keepdims=True)
                acc = acc + w * orecv[source, tile, :].astype(jnp.float32)
            outst[tile, :] = acc.astype(jnp.bfloat16)
        for j in near_first:
            to = (a + j) % side

            @pl.when(to // half == piece)
            def _():
                home(to, 0)
                home(to, 1)

        @pl.when(a // half == piece)
        def _():
            home(a, 1 - c)
            out[:, head_cols(own_head)] = outst[own_row, :]

    loop(1, side, part_arrived)
    for piece in range(2):
        piece_arrived(piece)
        finish(piece)

    ref = qall.at[0, pl.ds(0, others), :]
    pltpu.make_async_copy(ref, ref, p1_send.at[0]).wait()
    ref = kv.at[:, pl.ds(0, others), :]
    pltpu.make_async_copy(ref, ref, p1_send.at[1]).wait()

    for copy in first_hops + second_hops[2] + second_hops[side - 2]:
        copy.wait_send()

    def part_left(delta):
        chunk = (g + delta) % side

        @pl.when(delta != half)
        def _():
            part(0, chunk, g).wait_send()
            part(1, chunk, g).wait_send()

    loop(1, side, part_left)
    for kind, piece in halves:
        part(kind, opposite, g, piece).wait_send()
    ref = outst.at[pl.ds(0, others), :]
    pltpu.make_async_copy(ref, ref, p4_recv).wait()
    pltpu.make_async_copy(ref, ref, p4_send).wait()


def shards(queries, fresh_keys, fresh_values, stale_keys, stale_values, patch_sizes):
    local, columns = queries.shape
    chips = lax.axis_size("seq") // 2
    side = math.isqrt(chips)
    assert side * side == chips and columns == 2 * side * HEAD
    rows = 2 * side * local
    half = side // 2
    bf16, f32 = jnp.bfloat16, jnp.float32
    dma = pltpu.SemaphoreType.DMA
    return pl.pallas_call(
        functools.partial(kernel, side, local),
        out_shape=jax.ShapeDtypeStruct((local, columns), bf16),
        in_specs=[pl.BlockSpec(memory_space=pltpu.SMEM)] + [pl.BlockSpec(memory_space=pl.ANY)] * 5,
        out_specs=pl.BlockSpec(memory_space=pltpu.VMEM),
        scratch_shapes=[
            pltpu.VMEM((5, local, columns), bf16),
            pltpu.VMEM((side, rows, HEAD), bf16),
            pltpu.VMEM((4, rows, HEAD), bf16),
            pltpu.VMEM((rows, PATCHES * HEAD), bf16),
            pltpu.VMEM((rows, PATCHES * HEAD), bf16),
            pltpu.VMEM((side, rows, HEAD), bf16),
            pltpu.VMEM((side, rows // HEAD, HEAD), f32),
            pltpu.VMEM((side, rows, HEAD), bf16),
            pltpu.VMEM((side, rows // HEAD, HEAD), f32),
            pltpu.VMEM((rows, HEAD), bf16),
            dma((5,)),
            dma((5,)),
            dma((2,)),
            dma((2,)),
            pltpu.SemaphoreType.REGULAR((4 * side,)),
            dma((side,)),
            dma((side,)),
            dma((2, side + 1)),
            dma((2, side + 1)),
            dma,
            dma,
        ],
        compiler_params=pltpu.CompilerParams(collective_id=0, has_side_effects=True),
    )(patch_sizes, queries, fresh_keys, fresh_values, stale_keys, stale_values)


def solution(mesh):
    in_specs = (
        P(("groups", "seq"), None),
        P(("groups", "seq"), None),
        P(("groups", "seq"), None),
        P(("groups", "seq"), None),
        P(("groups", "seq"), None),
        P("groups"),
    )
    out_specs = P(("groups", "seq"), None)
    return jax.shard_map(shards, mesh=mesh, in_specs=in_specs, out_specs=out_specs, check_vma=False)
```

```python
import functools
import math

import jax
import jax.numpy as jnp
from jax import lax
from jax.experimental import pallas as pl
from jax.experimental.pallas import tpu as pltpu
from jax.sharding import PartitionSpec as P

HEAD = 128
SUBS = 4
PATCHES = 4
MESH = pl.DeviceIdType.MESH


def kernel(
    side,
    local,
    sizes,
    q_in,
    fk_in,
    fv_in,
    sk_in,
    sv_in,
    out,
    stage,
    qall,
    kv,
    kcat,
    vcat,
    opart,
    lpart,
    orecv,
    lrecv,
    outst,
    load_sem,
    self_sem,
    p1_send,
    p1_recv,
    ready,
    ring_send,
    ring_recv,
    part_send,
    part_recv,
    p4_send,
    p4_recv,
):
    group = lax.axis_index("groups")
    me = lax.axis_index("seq")
    c = me % 2
    x = (me // 2) % side
    y = me // 2 // side
    a = x * (1 - c) + y * c
    g = y * (1 - c) + x * c
    rows = 2 * side * local
    half = side // 2
    pair = 2 * local
    scale2 = (HEAD**-0.5) * math.log2(math.e)

    def at(cx, cy, core):
        return (group, (cy * side + cx) * 2 + core)

    def line(a_to, g_to, core):
        return at(a_to * (1 - c) + g_to * c, g_to * (1 - c) + a_to * c, core)

    def head_cols(head):
        return pl.ds(pl.multiple_of(head * HEAD, HEAD), HEAD)

    inputs = (q_in, fk_in, fv_in, sk_in, sv_in)
    loads = [pltpu.make_async_copy(ref, stage.at[i], load_sem.at[i]) for i, ref in enumerate(inputs)]
    loads[0].start()

    def block(index):
        return pl.ds(pl.multiple_of(index * local, local), local)

    def signal(semaphore, device):
        pl.semaphore_signal(semaphore, inc=1, device_id=device, device_id_type=MESH)

    def loop(first, last, body):
        def step(i, carry):
            body(i)
            return carry

        lax.fori_loop(first, last, step, 0)

    barrier = pltpu.get_barrier_semaphore()

    def greet_row(i):
        signal(barrier, at(i, y, 0))
        signal(barrier, at(i, y, 1))

    def greet_column(i):
        signal(barrier, at(x, i, 0))
        signal(barrier, at(x, i, 1))

    loop(0, x, greet_row)
    loop(0, y, greet_column)

    @pl.when(c == 1)
    def _():
        signal(barrier, at(x, y, 0))

    higher = 2 * (side - 1 - x) + 2 * (side - 1 - y) + (1 - c)

    @pl.when(higher > 0)
    def _():
        pl.semaphore_wait(barrier, higher)

    def ready_row(i):
        signal(ready.at[x * 2 + c], at(i, y, 0))
        signal(ready.at[x * 2 + c], at(i, y, 1))

    def ready_column(i):
        signal(ready.at[2 * side + y * 2 + c], at(x, i, 0))
        signal(ready.at[2 * side + y * 2 + c], at(x, i, 1))

    loop(x + 1, side, ready_row)
    loop(y + 1, side, ready_column)

    @pl.when(c == 0)
    def _():
        signal(ready.at[x * 2], at(x, y, 1))

    for copy in loads[1:]:
        copy.start()

    own_row = block(a * 2 + c)
    own_head = c * side + a
    own = []
    for i, ref in enumerate(inputs):
        dst = qall.at[g, own_row, :] if i == 0 else kv.at[i - 1, own_row, :]
        own.append(pltpu.make_async_copy(ref.at[:, head_cols(own_head)], dst, self_sem.at[i]))
        own[-1].start()

    row_x, row_y = block(x * 2 + c), block(y * 2 + c)

    def push(which, device, head, slot, row):
        if which == 0:
            src, dst = stage.at[0, :, head_cols(head)], qall.at[slot, row, :]
        else:
            src, dst = stage.at[pl.ds(1, 4), :, head_cols(head)], kv.at[:, row, :]
        pltpu.make_async_remote_copy(
            src_ref=src,
            dst_ref=dst,
            send_sem=p1_send.at[which],
            recv_sem=p1_recv.at[which],
            device_id=device,
            device_id_type=MESH,
        ).start()

    def push_row(which, i):
        push(which, at(i, y, 0), i, y, row_x)

    def push_column(which, i):
        push(which, at(x, i, 1), side + i, x, row_y)

    for which in range(2):
        for copy in loads[:1] if which == 0 else loads[1:]:
            copy.wait()
        loop(x + 1, side, functools.partial(push_row, which))
        loop(y + 1, side, functools.partial(push_column, which))

        @pl.when(c == 0)
        def _():
            push_column(which, y)

    def hear(index):
        pl.semaphore_wait(ready.at[index], 1)

    @pl.when(c == 1)
    def _():
        hear(x * 2)
        push_row(0, x)
        push_row(1, x)

    def lower_row(k):
        i = x - 1 - k
        hear(i * 2 + 1)
        hear(i * 2)
        push_row(0, i)
        push_row(1, i)

    def lower_column(k):
        i = y - 1 - k
        hear(2 * side + i * 2 + 1)
        push_column(0, i)
        push_column(1, i)
        hear(2 * side + i * 2)

    loop(0, x, lower_row)
    loop(0, y, lower_column)

    others = rows - local
    near_first = sorted(range(1, side), key=lambda i: min(i, side - i))

    def spread(delta, back=0, piece=None):
        chunk = (g + side - back) % side
        far = (delta + back) % side
        n = rows if piece is None else rows // 2
        ref = qall.at[chunk, pl.ds(0 if piece is None else piece * n, n), :]
        slot = far if piece != 1 else 0
        return pltpu.make_async_remote_copy(
            src_ref=ref,
            dst_ref=ref,
            send_sem=ring_send.at[slot],
            recv_sem=ring_recv.at[slot],
            device_id=line(a, (g + delta) % side, c),
            device_id_type=MESH,
        )

    def arrived(delta, piece=None):
        chunk = (g + side - delta) % side
        n = rows if piece is None else rows // 2
        ref = qall.at[chunk, pl.ds(0 if piece is None else piece * n, n), :]
        pltpu.make_async_copy(ref, ref, ring_recv.at[delta if piece != 1 else 0]).wait()

    firsts = (1, side - 1, 2, side - 2)
    first_hops = [spread(delta) for delta in firsts]
    second_hops = {
        2: [spread(1, 2), spread(2, 2, 0)],
        side - 2: [spread(side - 1, side - 2), spread(side - 2, side - 2, 1)],
    }

    own[0].wait()
    ref = qall.at[0, pl.ds(0, others), :]
    pltpu.make_async_copy(ref, ref, p1_recv.at[0]).wait()
    for copy in first_hops:
        copy.start()

    for copy in own[1:]:
        copy.wait()
    ref = kv.at[:, pl.ds(0, others), :]
    pltpu.make_async_copy(ref, ref, p1_recv.at[1]).wait()

    step_a = pair * (1 + c * (side - 1))
    step_g = pair * (side - c * (side - 1))
    end0 = sizes[0]
    end1 = end0 + sizes[1]
    end2 = end1 + sizes[2]

    def patches(count, start, chunk):
        l = lax.broadcasted_iota(jnp.int32, (count, HEAD), 0) + start
        pos = (l // pair) * step_a + chunk * step_g + l % pair
        one, zero = jnp.int32(1), jnp.int32(0)
        return sum(jnp.where(pos >= end, one, zero) for end in (end0, end1, end2))

    def indicator(mask):
        return jnp.where(mask, 1.0, 0.0).astype(jnp.bfloat16)

    key_patch = patches(rows, 0, g)
    for p in range(PATCHES):
        cols = pl.ds(p * HEAD, HEAD)
        fresh, stale = indicator(key_patch <= p), indicator(key_patch > p)
        kcat[:, cols] = kv[0] * fresh + kv[2] * stale
        vcat[:, cols] = kv[1] * fresh + kv[3] * stale

    eye = lax.broadcasted_iota(jnp.int32, (HEAD, HEAD), 0) == lax.broadcasted_iota(jnp.int32, (HEAD, HEAD), 1)
    contract = (((1,), (1,)), ((), ()))
    def compute(chunk, first=0, count=rows):
        q = qall[chunk, pl.ds(first, count), :]
        patch = patches(count, first, chunk)
        split = jnp.concatenate([q * indicator(patch == p) for p in range(PATCHES)], axis=1)
        s = lax.dot_general(split, kcat[...], contract, preferred_element_type=jnp.float32)
        m = jnp.max(s, axis=1, keepdims=True)
        w = jnp.exp2((s - m) * scale2)
        total = jnp.sum(w, axis=1, keepdims=True)
        o = jnp.dot(w.astype(jnp.bfloat16), vcat[...], preferred_element_type=jnp.float32)
        picked = o[:, :HEAD]
        for p in range(1, PATCHES):
            picked = jnp.where(patch == p, o[:, p * HEAD : (p + 1) * HEAD], picked)
        opart[chunk, pl.ds(first, count), :] = (picked / total).astype(jnp.bfloat16)
        lse = m * scale2 + jnp.log2(total)
        for k in range(count // HEAD):
            block_lse = lse[k * HEAD : (k + 1) * HEAD, :]
            lpart[chunk, pl.ds(first // HEAD + k, 1), :] = jnp.sum(jnp.where(eye, block_lse, 0.0), axis=0, keepdims=True)

    def part(kind, chunk, source, piece=None):
        src, dst = ((opart, orecv), (lpart, lrecv))[kind]
        n = src.shape[1]
        cut = pl.ds(0, n) if piece is None else pl.ds(piece * (n // 2), n // 2)
        extra = piece == 1
        return pltpu.make_async_remote_copy(
            src_ref=src.at[chunk, cut],
            dst_ref=dst.at[source, cut],
            send_sem=part_send.at[kind, side if extra else chunk],
            recv_sem=part_recv.at[kind, side if extra else source],
            device_id=line(a, chunk, c),
            device_id_type=MESH,
        )

    def do_part(delta):
        chunk = (g + side - delta) % side
        compute(chunk)
        part(0, chunk, g).start()
        part(1, chunk, g).start()

    def pass_on(delta):
        arrived(delta)
        for copy in second_hops[delta]:
            copy.start()

    compute(g)
    for delta in (1, side - 1):
        arrived(delta)
        do_part(delta)
    pass_on(2)
    pass_on(side - 2)
    do_part(2)
    do_part(side - 2)
    for delta in (3, side - 3):
        arrived(delta)
        do_part(delta)
    opposite = (g + half) % side
    halves = [(kind, piece) for piece in range(2) for kind in range(2)]
    for piece in range(2):
        arrived(half, piece)
        compute(opposite, piece * (rows // 2), rows // 2)
        for kind in range(2):
            part(kind, opposite, g, piece).start()

    orecv[g] = opart[g]
    lrecv[g] = lpart[g]

    def part_arrived(delta):
        source = (g + delta) % side

        @pl.when(delta != half)
        def _():
            pltpu.make_async_copy(orecv.at[source], orecv.at[source], part_recv.at[0, source]).wait()
            pltpu.make_async_copy(lrecv.at[source], lrecv.at[source], part_recv.at[1, source]).wait()

    def piece_arrived(piece):
        for kind, ref in enumerate((orecv, lrecv)):
            n = ref.shape[1] // 2
            cut = ref.at[opposite, pl.ds(piece * n, n)]
            pltpu.make_async_copy(cut, cut, part_recv.at[kind, side if piece else opposite]).wait()

    def home(a_to, core):
        pltpu.make_async_remote_copy(
            src_ref=outst.at[block(a_to * 2 + core), :],
            dst_ref=out.at[:, head_cols(own_head)],
            send_sem=p4_send,
            recv_sem=p4_recv,
            device_id=line(a_to, g, core),
            device_id_type=MESH,
        ).start()

    def finish(piece):
        n = rows // HEAD // 2
        lse = [lrecv[source, pl.ds(piece * n, n)] for source in range(side)]
        top = functools.reduce(jnp.maximum, lse)
        weights = [jnp.exp2(l - top) for l in lse]
        total = functools.reduce(jnp.add, weights)
        weights = [w / total for w in weights]
        for k in range(n):
            tile = pl.ds((piece * n + k) * HEAD, HEAD)
            acc = jnp.zeros((HEAD, HEAD), jnp.float32)
            for source in range(side):
                w = jnp.sum(jnp.where(eye, weights[source][k : k + 1, :], 0.0), axis=1, keepdims=True)
                acc = acc + w * orecv[source, tile, :].astype(jnp.float32)
            outst[tile, :] = acc.astype(jnp.bfloat16)
        for j in near_first:
            to = (a + j) % side

            @pl.when(to // half == piece)
            def _():
                home(to, 0)
                home(to, 1)

        @pl.when(a // half == piece)
        def _():
            home(a, 1 - c)
            out[:, head_cols(own_head)] = outst[own_row, :]

    loop(1, side, part_arrived)
    for piece in range(2):
        piece_arrived(piece)
        finish(piece)

    ref = qall.at[0, pl.ds(0, others), :]
    pltpu.make_async_copy(ref, ref, p1_send.at[0]).wait()
    ref = kv.at[:, pl.ds(0, others), :]
    pltpu.make_async_copy(ref, ref, p1_send.at[1]).wait()

    for copy in first_hops + second_hops[2] + second_hops[side - 2]:
        copy.wait_send()

    def part_left(delta):
        chunk = (g + delta) % side

        @pl.when(delta != half)
        def _():
            part(0, chunk, g).wait_send()
            part(1, chunk, g).wait_send()

    loop(1, side, part_left)
    for kind, piece in halves:
        part(kind, opposite, g, piece).wait_send()
    ref = outst.at[pl.ds(0, others), :]
    pltpu.make_async_copy(ref, ref, p4_recv).wait()
    pltpu.make_async_copy(ref, ref, p4_send).wait()


def shards(queries, fresh_keys, fresh_values, stale_keys, stale_values, patch_sizes):
    local, columns = queries.shape
    chips = lax.axis_size("seq") // 2
    side = math.isqrt(chips)
    assert side * side == chips and columns == 2 * side * HEAD
    rows = 2 * side * local
    half = side // 2
    bf16, f32 = jnp.bfloat16, jnp.float32
    dma = pltpu.SemaphoreType.DMA
    return pl.pallas_call(
        functools.partial(kernel, side, local),
        out_shape=jax.ShapeDtypeStruct((local, columns), bf16),
        in_specs=[pl.BlockSpec(memory_space=pltpu.SMEM)] + [pl.BlockSpec(memory_space=pl.ANY)] * 5,
        out_specs=pl.BlockSpec(memory_space=pltpu.VMEM),
        scratch_shapes=[
            pltpu.VMEM((5, local, columns), bf16),
            pltpu.VMEM((side, rows, HEAD), bf16),
            pltpu.VMEM((4, rows, HEAD), bf16),
            pltpu.VMEM((rows, PATCHES * HEAD), bf16),
            pltpu.VMEM((rows, PATCHES * HEAD), bf16),
            pltpu.VMEM((side, rows, HEAD), bf16),
            pltpu.VMEM((side, rows // HEAD, HEAD), f32),
            pltpu.VMEM((side, rows, HEAD), bf16),
            pltpu.VMEM((side, rows // HEAD, HEAD), f32),
            pltpu.VMEM((rows, HEAD), bf16),
            dma((5,)),
            dma((5,)),
            dma((2,)),
            dma((2,)),
            pltpu.SemaphoreType.REGULAR((4 * side,)),
            dma((side,)),
            dma((side,)),
            dma((2, side + 1)),
            dma((2, side + 1)),
            dma,
            dma,
        ],
        compiler_params=pltpu.CompilerParams(collective_id=0, has_side_effects=True),
    )(patch_sizes, queries, fresh_keys, fresh_values, stale_keys, stale_values)


def solution(mesh):
    in_specs = (
        P(("groups", "seq"), None),
        P(("groups", "seq"), None),
        P(("groups", "seq"), None),
        P(("groups", "seq"), None),
        P(("groups", "seq"), None),
        P("groups"),
    )
    out_specs = P(("groups", "seq"), None)
    return jax.shard_map(shards, mesh=mesh, in_specs=in_specs, out_specs=out_specs, check_vma=False)
```
